256 devices in a mesh: grp: 4 (over z_lo), slab: 64 (over z_hi, x, y, core).
Axes of the slice: x: 4, y: 4, z: 8 (z_hi: 2, z_lo: 4; z = z_hi * 4 + z_lo), core: 2. Of those that a mesh axis runs over, the one named last changes fastest.
Arguments:
- snapshots: bfloat16 [4, 128, 256, 8, 128], P('grp', None, 'slab'), may hold values from -24 to 24
- base_flow: float32 [256, 8, 128], P('slab'), may hold values from 0.1 to 0.6
Outputs:
- direct_modes: bfloat16 [128, 256, 8, 128], P('grp', 'slab')
- adjoint_modes: bfloat16 [128, 256, 8, 128], P('grp', 'slab')
The draws below stay inside these ranges and needn't reach their ends.
All inputs are finite; a program needn't handle non-finite values.
Results may differ from the reference program's by a relative error of at most 0.015.
Values may be sent and summed in bfloat16 or wider, within the bound.
A program may use at most 64 MiB of HBM per device.

```python
import math
import jax
import jax.numpy as jnp
from jax import lax

NY = 8
NZ = 128
SNAP = 128
SECTIONS = 4
NX = 256
N_GRP = 4


def shard_levels(stream_key, dims, cuts, smallest, top_value):
    def one(axis_at, shards_of):
        heights = jax.random.uniform(jax.random.fold_in(jax.random.fold_in(stream_key, 6), axis_at), (shards_of,), jnp.float32, smallest / len(cuts), top_value / len(cuts))
        return jnp.repeat(jnp.exp(heights), dims[axis_at] // shards_of).reshape((-1,) + (1,) * (len(dims) - axis_at - 1))

    gain = one(*cuts[0])
    for cut in cuts[1:]:
        gain = gain * one(*cut)
    return gain


def noise(key, extent, spread, most, split=(), kind=jnp.bfloat16):
    gain = shard_levels(key, extent, split, -0.22, 0.18) if split else 1.0
    result = jax.random.normal(key, extent, jnp.float32) * spread * gain
    return jnp.minimum(jnp.maximum(result, -most), most).astype(kind)


def setup_inputs(seed: int = 0) -> dict:
    streams_of = jax.random.split(jax.random.key(seed), 3)
    snapshots = noise(streams_of[0], (N_GRP, SNAP, NX, NY, NZ), 4.0, 24.0, ((0, 4), (2, 64)))
    base_flow = jnp.clip(0.1 + 0.5 * jax.random.uniform(streams_of[1], (NX, NY, NZ), jnp.float32) ** shard_levels(streams_of[1], (NX, NY, NZ), ((0, 64),), -0.2, 0.2), 0.1, 0.6)
    return dict(snapshots=snapshots, base_flow=base_flow)


diffuse_x = 0.35
diffuse_side = 0.05
keep_center = 0.1
damping = 0.5

def advance(snapshot_field, plus_coef, minus_coef):
    block_size = math.gcd(SNAP, 16)
    blocks = snapshot_field.reshape((SNAP // block_size, block_size) + snapshot_field.shape[1:])

    def sweep_block(snap_block):
        for section_index in range(SECTIONS):
            center = snap_block.astype(jnp.float32)
            ahead_cells = jnp.roll(center, -1, axis=1)
            behind = jnp.roll(center, 1, axis=1)
            side_sum = jnp.roll(center, 1, axis=2) + jnp.roll(center, -1, axis=2)
            side_sum = side_sum + jnp.roll(center, 1, axis=3) + jnp.roll(center, -1, axis=3)
            updated = keep_center * center + plus_coef * ahead_cells + minus_coef * behind + diffuse_side * side_sum
            snap_block = updated.astype(jnp.bfloat16)
        return snap_block
    return lax.map(sweep_block, blocks).reshape(snapshot_field.shape)

def reference(snapshots, base_flow):
    plus_direct = diffuse_x - 0.5 * base_flow
    minus_direct = diffuse_x + 0.5 * base_flow
    plus_adjoint = diffuse_x + 0.5 * jnp.roll(base_flow, -1, axis=0)
    minus_adjoint = diffuse_x - 0.5 * jnp.roll(base_flow, 1, axis=0)
    adjoint = advance(snapshots[N_GRP - 1], plus_adjoint, minus_adjoint).reshape(SNAP, -1)
    norm_scale = 1.0 / math.sqrt(NX * NY * NZ)
    directs = []
    couplings = []
    gram_matrix = jnp.zeros((SNAP, SNAP), jnp.float32)
    for group_index in range(N_GRP - 1):
        direct = advance(snapshots[group_index], plus_direct, minus_direct).reshape(SNAP, -1)
        coupling = lax.dot_general(adjoint.astype(jnp.float32), direct.astype(jnp.float32), (((1,), (1,)), ((), ())), preferred_element_type=jnp.float32) * norm_scale
        gram_matrix = gram_matrix + jnp.dot(coupling, coupling.T, precision=lax.Precision.HIGHEST)
        directs.append(direct)
        couplings.append(coupling)
    energy = jnp.trace(gram_matrix) / SNAP
    system = gram_matrix / energy + damping * jnp.eye(SNAP, dtype=jnp.float32)
    factor = jnp.linalg.cholesky(system)
    inverse = jax.scipy.linalg.cho_solve((factor, True), jnp.eye(SNAP, dtype=jnp.float32))
    total_modes = jnp.zeros((SNAP, NX * NY * NZ), jnp.float32)
    for group_index in range(N_GRP - 1):
        weights = (jnp.dot(inverse, couplings[group_index], precision=lax.Precision.HIGHEST) / jnp.sqrt(energy)).astype(jnp.bfloat16)
        mode_term = jnp.dot(weights.astype(jnp.float32), directs[group_index].astype(jnp.float32), preferred_element_type=jnp.float32)
        total_modes = total_modes + lax.optimization_barrier(mode_term.astype(jnp.bfloat16)).astype(jnp.float32)
    direct_modes = total_modes.astype(jnp.bfloat16).reshape(SNAP, NX, NY, NZ)
    adjoint_modes = jnp.dot(inverse.astype(jnp.bfloat16).astype(jnp.float32), adjoint.astype(jnp.float32), preferred_element_type=jnp.float32)
    adjoint_modes = adjoint_modes.astype(jnp.bfloat16).reshape(SNAP, NX, NY, NZ)
    return (direct_modes, adjoint_modes)
```

```python
import functools
import math

import jax
import jax.numpy as jnp
from jax import lax
from jax.experimental import pallas as pl
from jax.experimental.pallas import tpu as pltpu
from jax.sharding import PartitionSpec as P

SNAP = 128
SECTIONS = 4
CHUNKS = 8
PER = SNAP // CHUNKS
MESH = pl.DeviceIdType.MESH
MIB = 1 << 20

diffuse_x = 0.35
diffuse_side = 0.05
keep_center = 0.1
damping = 0.5


def remote(src, dst, send_sem, recv_sem, device):
    return pltpu.make_async_remote_copy(
        src_ref=src, dst_ref=dst, send_sem=send_sem, recv_sem=recv_sem, device_id=device, device_id_type=MESH
    )


def place():
    g = lax.axis_index("grp")
    s = lax.axis_index("slab")
    core = lax.rem(s, 2)
    plane = lax.rem(lax.div(s, 2), 16)
    zh = lax.div(s, 32)
    return g, s, core, plane, zh


def slab_of(zh, plane, core):
    return zh * 32 + plane * 2 + core


def gather_kernel(
    scale,
    u_ref,
    v_ref,
    direct_ref,
    adj_ref,
    coup_ref,
    left,
    right,
    vleft,
    vright,
    cp,
    cm,
    stage,
    part,
    rs_buf,
    tile,
    zbuf,
    mine,
    h_send,
    h_recv,
    v_send,
    v_recv,
    a_send,
    a_recv,
    p_send,
    p_recv,
    z_send,
    z_recv,
    g_send,
    g_recv,
):
    g, s, core, plane, zh = place()
    ahead = lax.rem(s + 1, 64)
    back = lax.rem(s + 63, 64)
    adjoint = g == 3

    barrier = pltpu.get_barrier_semaphore()
    for other in (ahead, back):
        pl.semaphore_signal(barrier, inc=1, device_id=(g, other), device_id_type=MESH)
    for d in range(1, 16):
        pl.semaphore_signal(
            barrier, inc=1, device_id=(g, slab_of(zh, lax.rem(plane + d, 16), core)), device_id_type=MESH
        )
    for d in range(1, 16):
        g2 = lax.rem(g + d // 4, 4)
        zh2 = lax.rem(zh + (d // 2) % 2, 2)
        c2 = lax.rem(core + d % 2, 2)
        pl.semaphore_signal(barrier, inc=1, device_id=(g2, slab_of(zh2, plane, c2)), device_id_type=MESH)
    pl.semaphore_wait(barrier, 32)

    flow = [
        remote(v_ref, vleft, v_send.at[0], v_recv.at[0], (g, ahead)),
        remote(v_ref, vright, v_send.at[1], v_recv.at[1], (g, back)),
    ]
    for copy in flow:
        copy.start()

    def halo(c):
        rows = pl.ds(c * PER, PER)
        return [
            remote(u_ref.at[rows], left.at[rows], h_send.at[0, c], h_recv.at[0, c], (g, ahead)),
            remote(u_ref.at[rows], right.at[rows], h_send.at[1, c], h_recv.at[1, c], (g, back)),
        ]

    def start_halo(c, carry):
        for copy in halo(c):
            copy.start()
        return carry

    lax.fori_loop(0, CHUNKS, start_halo, 0)
    for copy in flow:
        copy.wait()

    v = [vleft[k] for k in range(4)] + [v_ref[k] for k in range(4)] + [vright[k] for k in range(4)]
    for k in range(10):
        cp[k] = jnp.where(adjoint, diffuse_x + 0.5 * v[k + 2], diffuse_x - 0.5 * v[k + 1])
        cm[k] = jnp.where(adjoint, diffuse_x - 0.5 * v[k], diffuse_x + 0.5 * v[k + 1])

    def sections(snap, base):
        rows = [ref[snap, k].astype(jnp.float32) for ref in (left, u_ref, right) for k in range(4)]
        for section in range(SECTIONS):
            new = []
            for k in range(len(rows) - 2):
                center = rows[k + 1]
                side = pltpu.roll(center, 1, 0) + pltpu.roll(center, 7, 0)
                side = side + pltpu.roll(center, 1, 1) + pltpu.roll(center, 127, 1)
                new.append(
                    keep_center * center
                    + cp[section + k] * rows[k + 2]
                    + cm[section + k] * rows[k]
                    + diffuse_side * side
                )
            rows = new
        for k in range(4):
            stage[pl.ds(base + k * 64, 8, stride=8), :] = rows[k]

    def chain(c):
        return remote(
            adj_ref.at[c], adj_ref.at[c], a_send.at[c], a_recv.at[c], (lax.max(g - 1, 0), s)
        )

    def relay(c):
        @pl.when((g == 1) | (g == 2))
        def _():
            chain(c).wait_recv()
            chain(c).start()

    def chunk(c, carry):
        for copy in halo(c):
            copy.wait_recv()

        def one(i, inner):
            for half in range(2):
                sections(c * PER + half * 8 + i, half * 256 + i)
            return inner

        lax.fori_loop(0, 8, one, 0)

        def packed(q):
            low = stage[q * 8 : q * 8 + 8, :]
            high = stage[256 + q * 8 : 256 + q * 8 + 8, :]
            return jnp.concatenate([low, high], axis=0).astype(jnp.bfloat16)

        @pl.when(adjoint)
        def _():
            for q in range(32):
                adj_ref[c, q] = packed(q)
            chain(c).start()

        @pl.when(jnp.logical_not(adjoint))
        def _():
            for q in range(32):
                direct_ref[c, q] = packed(q)

        @pl.when(c >= 1)
        def _():
            relay(c - 1)

        return carry

    lax.fori_loop(0, CHUNKS, chunk, 0)
    relay(CHUNKS - 1)

    @pl.when(g == 0)
    def _():
        for c in range(CHUNKS):
            chain(c).wait_recv()

    def plane_peer(d):
        return lax.rem(plane + d, 16)

    def scatter(d):
        p2 = plane_peer(d)
        return remote(
            part.at[p2], rs_buf.at[plane], p_send.at[p2], p_recv.at[plane], (g, slab_of(zh, p2, core))
        )

    def scatter_in(d):
        p2 = plane_peer(d)
        return remote(
            part.at[plane], rs_buf.at[p2], p_send.at[plane], p_recv.at[p2], (g, slab_of(zh, p2, core))
        )

    slot = g * 4 + zh * 2 + core

    def peer16(d):
        g2 = lax.rem(g + d // 4, 4)
        zh2 = lax.rem(zh + (d // 2) % 2, 2)
        c2 = lax.rem(core + d % 2, 2)
        return g2, zh2, c2

    def spread(d):
        g2, zh2, c2 = peer16(d)
        return remote(
            tile, zbuf.at[slot], z_send.at[d], z_recv.at[slot], (g2, slab_of(zh2, plane, c2))
        )

    @pl.when(jnp.logical_not(adjoint))
    def _():
        def product(q, acc):
            lhs = [adj_ref[:, 2 * q + j].reshape(SNAP, 128) for j in range(2)]
            rhs = [direct_ref[:, 2 * q + j].reshape(SNAP, 128) for j in range(2)]
            return acc + lax.dot_general(
                jnp.concatenate(lhs, axis=1),
                jnp.concatenate(rhs, axis=1),
                (((1,), (1,)), ((), ())),
                preferred_element_type=jnp.float32,
            )

        total = lax.fori_loop(0, 16, product, jnp.zeros((SNAP, SNAP), jnp.float32))
        part[...] = total.reshape(16, 8, SNAP)
        for d in range(1, 16):
            scatter(d).start()
        rs_buf[plane] = part[plane]
        for d in range(1, 16):
            scatter_in(d).wait_recv()
        tile[...] = jnp.sum(rs_buf[...], axis=0)
        for d in range(1, 16):
            spread(d).start()
        zbuf[slot] = tile[...]

    for g2 in range(3):
        for k in range(4):
            here = g2 * 4 + k

            @pl.when(slot != here)
            def _():
                pltpu.make_async_copy(zbuf.at[here], zbuf.at[here], z_recv.at[here]).wait()

    for g2 in range(3):
        mine[g2] = jnp.sum(zbuf[g2 * 4 : g2 * 4 + 4], axis=0) * scale

    def share(d):
        p2 = plane_peer(d)
        return remote(
            mine, coup_ref.at[plane], g_send.at[p2], g_recv.at[plane], (g, slab_of(zh, p2, core))
        )

    def share_in(d):
        p2 = plane_peer(d)
        return remote(mine, coup_ref.at[p2], g_send.at[plane], g_recv.at[p2], (g, slab_of(zh, p2, core)))

    for d in range(1, 16):
        share(d).start()
    coup_ref[plane] = mine[...]
    for d in range(1, 16):
        share_in(d).wait_recv()

    def drain(c, carry):
        for copy in halo(c):
            copy.wait_send()

        @pl.when(g > 0)
        def _():
            chain(c).wait_send()

        return carry

    lax.fori_loop(0, CHUNKS, drain, 0)
    for d in range(1, 16):
        share(d).wait_send()

    @pl.when(jnp.logical_not(adjoint))
    def _():
        for d in range(1, 16):
            scatter(d).wait_send()
            spread(d).wait_send()


def inverse_kernel(coup_ref, weights_ref, inverse_ref, m_ref):
    g = lax.axis_index("grp")
    gram = jnp.zeros((SNAP, SNAP), jnp.float32)
    for k in range(3):
        c = coup_ref[:, k].reshape(SNAP, SNAP)
        gram = gram + lax.dot_general(
            c, c, (((1,), (1,)), ((), ())), precision=lax.Precision.HIGHEST, preferred_element_type=jnp.float32
        )
    row = lax.broadcasted_iota(jnp.int32, (SNAP, SNAP), 0)
    col = lax.broadcasted_iota(jnp.int32, (SNAP, SNAP), 1)
    eye = (row == col).astype(jnp.float32)
    energy = jnp.sum(gram * eye, axis=(0, 1), keepdims=True) / SNAP
    m_ref[...] = gram / energy + damping * eye

    sub = lax.broadcasted_iota(jnp.int32, (8, SNAP), 0)
    lane = lax.broadcasted_iota(jnp.int32, (8, SNAP), 1)

    def spread_row(x, j):
        return jnp.broadcast_to(x[j : j + 1, :], (8, SNAP))

    for b in range(16):
        full = m_ref[...]
        columns = [jnp.broadcast_to(full[:, 8 * b + j : 8 * b + j + 1], (SNAP, SNAP)) for j in range(8)]
        panel = full[8 * b : 8 * b + 8, :]
        pivots = [c[8 * b : 8 * b + 8, :] for c in columns]
        for j in range(8):
            own = sub == j
            inv = 1.0 / spread_row(pivots[j], j)
            pj = pivots[j]
            panel = jnp.where(lane == 8 * b + j, own.astype(jnp.float32), panel)
            new = spread_row(panel, j) * inv
            panel = jnp.where(own, new, panel - pj * new)
            for i in range(j + 1, 8):
                new = spread_row(pivots[i], j) * inv
                pivots[i] = jnp.where(own, new, pivots[i] - pj * new)
        inside = (lane >= 8 * b) & (lane < 8 * b + 8)
        spread = [spread_row(panel, j) for j in range(8)]
        for t in range(16):
            if t == b:
                m_ref[8 * t : 8 * t + 8, :] = panel
            else:
                rest = jnp.where(inside, 0.0, full[8 * t : 8 * t + 8, :])
                for j in range(8):
                    rest = rest - columns[j][8 * t : 8 * t + 8, :] * spread[j]
                m_ref[8 * t : 8 * t + 8, :] = rest
    inverse = m_ref[...]
    inverse_ref[...] = inverse.astype(jnp.bfloat16)
    own = coup_ref[:, lax.min(g, 2)].reshape(SNAP, SNAP)
    weights = jnp.dot(
        inverse, own, precision=lax.Precision.HIGHEST, preferred_element_type=jnp.float32
    ) / jnp.sqrt(energy)
    weights_ref[...] = weights.astype(jnp.bfloat16)


def modes_kernel(
    direct_ref, adj_ref, weights_ref, inverse_ref, dm_ref, am_ref, terms, inbox, t_send, t_recv
):
    g, s, core, plane, zh = place()
    adjoint = g == 3
    barrier = pltpu.get_barrier_semaphore()
    for d in range(1, 4):
        pl.semaphore_signal(barrier, inc=1, device_id=(lax.rem(g + d, 4), s), device_id_type=MESH)

    def rows_of(ref, q):
        return ref[:, q].reshape(SNAP, 128)

    @pl.when(jnp.logical_not(adjoint))
    def _():
        def product(q, carry):
            rhs = jnp.concatenate([rows_of(direct_ref, 2 * q + j) for j in range(2)], axis=1)
            out = jnp.dot(weights_ref[...], rhs, preferred_element_type=jnp.float32).astype(jnp.bfloat16)
            for j in range(2):
                terms[:, 2 * q + j] = out[:, j * 128 : j * 128 + 128].reshape(4, 32, 128)
            return carry

        lax.fori_loop(0, 16, product, 0)

    pl.semaphore_wait(barrier, 3)

    def send(r):
        return remote(terms.at[r], inbox.at[g], t_send.at[r], t_recv.at[g], (r, s))

    for r in (3, 0, 2, 1):

        @pl.when(jnp.logical_not(adjoint) & (g != r))
        def _():
            send(r).start()

    own = inverse_ref[pl.ds(pl.multiple_of(g * 32, 32), 32), :]

    def adjoint_product(q, carry):
        rhs = jnp.concatenate([rows_of(adj_ref, 2 * q + j) for j in range(2)], axis=1)
        out = jnp.dot(own, rhs, preferred_element_type=jnp.float32).astype(jnp.bfloat16)
        for j in range(2):
            am_ref[2 * q + j] = out[:, j * 128 : j * 128 + 128]
        return carry

    lax.fori_loop(0, 16, adjoint_product, 0)

    for k in range(3):

        @pl.when(g != k)
        def _():
            pltpu.make_async_copy(inbox.at[k], inbox.at[k], t_recv.at[k]).wait()

        @pl.when(g == k)
        def _():
            inbox[k] = terms[k]

    def total(q, carry):
        acc = inbox[0, q].astype(jnp.float32)
        for k in (1, 2):
            acc = acc + inbox[k, q].astype(jnp.float32)
        dm_ref[q] = acc.astype(jnp.bfloat16)
        return carry

    lax.fori_loop(0, 32, total, 0, unroll=4)
    for r in range(4):

        @pl.when(jnp.logical_not(adjoint) & (g != r))
        def _():
            send(r).wait_send()


def per_device(snapshots, base_flow):
    field = snapshots[0]
    f32, bf16 = jnp.float32, jnp.bfloat16
    vmem = pl.BlockSpec(memory_space=pltpu.VMEM)
    dma = pltpu.SemaphoreType.DMA
    slab_shape = field.shape
    cells = 64 * math.prod(slab_shape[1:])
    scale = 1.0 / math.sqrt(cells)
    packed = jax.ShapeDtypeStruct((CHUNKS, 32, PER, 128), bf16)
    direct, adj, coup = pl.pallas_call(
        functools.partial(gather_kernel, scale),
        out_shape=(packed, packed, jax.ShapeDtypeStruct((16, 3, 8, SNAP), f32)),
        in_specs=[vmem] * 2,
        out_specs=(vmem,) * 3,
        scratch_shapes=[
            pltpu.VMEM(slab_shape, bf16),
            pltpu.VMEM(slab_shape, bf16),
            pltpu.VMEM((4, 8, 128), f32),
            pltpu.VMEM((4, 8, 128), f32),
            pltpu.VMEM((10, 8, 128), f32),
            pltpu.VMEM((10, 8, 128), f32),
            pltpu.VMEM((512, 128), f32),
            pltpu.VMEM((16, 8, SNAP), f32),
            pltpu.VMEM((16, 8, SNAP), f32),
            pltpu.VMEM((8, SNAP), f32),
            pltpu.VMEM((12, 8, SNAP), f32),
            pltpu.VMEM((3, 8, SNAP), f32),
            dma((2, CHUNKS)),
            dma((2, CHUNKS)),
            dma((2,)),
            dma((2,)),
            dma((CHUNKS,)),
            dma((CHUNKS,)),
            dma((16,)),
            dma((16,)),
            dma((16,)),
            dma((12,)),
            dma((16,)),
            dma((16,)),
        ],
        compiler_params=pltpu.CompilerParams(
            collective_id=0, has_side_effects=True, vmem_limit_bytes=40 * MIB
        ),
        name="gather",
    )(field, base_flow)
    weights, inverse = pl.pallas_call(
        inverse_kernel,
        out_shape=(jax.ShapeDtypeStruct((SNAP, SNAP), bf16),) * 2,
        in_specs=[vmem],
        out_specs=(vmem,) * 2,
        scratch_shapes=[pltpu.VMEM((SNAP, SNAP), f32)],
        name="inverse",
    )(coup)
    modes = jax.ShapeDtypeStruct((32, 32, 128), bf16)
    dm, am = pl.pallas_call(
        modes_kernel,
        out_shape=(modes, modes),
        in_specs=[vmem] * 4,
        out_specs=(vmem,) * 2,
        scratch_shapes=[
            pltpu.VMEM((4, 32, 32, 128), bf16),
            pltpu.VMEM((3, 32, 32, 128), bf16),
            dma((4,)),
            dma((3,)),
        ],
        compiler_params=pltpu.CompilerParams(
            collective_id=1, has_side_effects=True, vmem_limit_bytes=40 * MIB
        ),
        name="modes",
    )(direct, adj, weights, inverse)

    def placed(x):
        return x.reshape(4, 8, 32, 128).transpose(2, 0, 1, 3)

    return placed(dm), placed(am)


def solution(mesh):
    return jax.shard_map(
        per_device,
        mesh=mesh,
        in_specs=(P("grp", None, "slab", None, None), P("slab", None, None)),
        out_specs=(P("grp", "slab", None, None), P("grp", "slab", None, None)),
        check_vma=False,
    )
```

```python
import functools
import math

import jax
import jax.numpy as jnp
from jax import lax
from jax.experimental import pallas as pl
from jax.experimental.pallas import tpu as pltpu
from jax.sharding import PartitionSpec as P

SNAP = 128
SECTIONS = 4
CHUNKS = 8
PER = SNAP // CHUNKS
MESH = pl.DeviceIdType.MESH
MIB = 1 << 20
EARLY = 2

diffuse_x = 0.35
diffuse_side = 0.05
keep_center = 0.1
damping = 0.5


def remote(src, dst, send_sem, recv_sem, device):
    return pltpu.make_async_remote_copy(
        src_ref=src, dst_ref=dst, send_sem=send_sem, recv_sem=recv_sem, device_id=device, device_id_type=MESH
    )


def place():
    g = lax.axis_index("grp")
    s = lax.axis_index("slab")
    core = lax.rem(s, 2)
    plane = lax.rem(lax.div(s, 2), 16)
    zh = lax.div(s, 32)
    return g, s, core, plane, zh


def slab_of(zh, plane, core):
    return zh * 32 + plane * 2 + core


def kernel(
    scale,
    u_ref,
    v_ref,
    dm_ref,
    am_ref,
    left,
    right,
    relay_buf,
    vleft,
    vright,
    cp,
    cm,
    stage,
    fields,
    adj_ref,
    part,
    rs_buf,
    tile,
    zbuf,
    mine,
    coup_ref,
    m_ref,
    acc,
    terms,
    inbox,
    h_send,
    h_recv,
    v_send,
    v_recv,
    x_send,
    x_recv,
    y_send,
    y_recv,
    a_send,
    a_recv,
    up_send,
    down_send,
    far_send,
    d_recv,
    p_send,
    p_recv,
    z_send,
    z_recv,
    g_send,
    g_recv,
    t_send,
    t_recv,
):
    g, s, core, plane, zh = place()
    ahead = lax.rem(s + 1, 64)
    back = lax.rem(s + 63, 64)
    adjoint = g == 3
    direct = g < 3
    middle = (g == 1) | (g == 2)
    z = zh * 4 + g
    last = (plane == 15) & (core == 1)
    first = (plane == 0) & (core == 0)
    edge = last | first

    def at(depth, position, side):
        depth = lax.rem(depth, 8)
        return lax.rem(depth, 4), slab_of(lax.div(depth, 4), position, side)

    def peer16(d):
        g2 = lax.rem(g + d // 4, 4)
        zh2 = lax.rem(zh + (d // 2) % 2, 2)
        c2 = lax.rem(core + d % 2, 2)
        return g2, slab_of(zh2, plane, c2)

    def plane_peer(d):
        return lax.rem(plane + d, 16)

    barrier = pltpu.get_barrier_semaphore()

    def greet(device):
        pl.semaphore_signal(barrier, inc=1, device_id=device, device_id_type=MESH)

    greet((g, ahead))
    greet((g, back))
    for d in range(1, 16):
        greet((g, slab_of(zh, plane_peer(d), core)))
        greet(peer16(d))

    far_end = at(z + 4, 15 * (1 - core), 1 - core)
    greet(far_end)

    @pl.when(edge)
    def _():
        def one(i, carry):
            greet(at(z + 4, i, 1 - core))
            return carry

        lax.fori_loop(0, 16, one, 0)

    pl.semaphore_wait(barrier, 33 + jnp.where(edge, 16, 0))

    flow = [
        remote(v_ref, vleft, v_send.at[0], v_recv.at[0], (g, ahead)),
        remote(v_ref, vright, v_send.at[1], v_recv.at[1], (g, back)),
    ]
    for copy in flow:
        copy.start()

    def rows(c):
        return pl.ds(c * PER, PER)

    def halo(c):
        return [
            remote(u_ref.at[rows(c)], left.at[rows(c)], h_send.at[0, c], h_recv.at[0, c], (g, ahead)),
            remote(u_ref.at[rows(c)], right.at[rows(c)], h_send.at[1, c], h_recv.at[1, c], (g, back)),
        ]

    def half(i):
        return pl.ds(i * 8, 8)

    def to_relay(i):
        return remote(u_ref.at[half(i)], relay_buf, x_send.at[i], y_recv, (g, slab_of(zh, i, core)))

    def across(src, i, send_sem):
        return (
            remote(src, right.at[half(i)], send_sem, x_recv.at[i], far_end),
            remote(src, left.at[half(i)], send_sem, x_recv.at[i], far_end),
        )

    def start_across(src, i, send_sem):
        to_right, to_left = across(src, i, send_sem)

        @pl.when(core == 0)
        def _():
            to_right.start()

        @pl.when(core == 1)
        def _():
            to_left.start()

    @pl.when(edge)
    def _():
        def one(i, carry):
            @pl.when(i != plane)
            def _():
                to_relay(i).start()

            @pl.when(i == plane)
            def _():
                start_across(u_ref.at[half(i)], i, x_send.at[i])

            return carry

        lax.fori_loop(0, 16, one, 0)

    def start_halo(c, carry):
        ahead_copy, back_copy = halo(c)

        @pl.when(jnp.logical_not(last))
        def _():
            ahead_copy.start()

        @pl.when(jnp.logical_not(first))
        def _():
            back_copy.start()

        return carry

    lax.fori_loop(0, CHUNKS, start_halo, 0)

    def pass_on():
        pltpu.make_async_copy(relay_buf, relay_buf, y_recv).wait()
        start_across(relay_buf, plane, y_send)

    def halo_in(c):
        ahead_copy, back_copy = halo(c)

        @pl.when(jnp.logical_not(first))
        def _():
            ahead_copy.wait_recv()

        @pl.when(jnp.logical_not(last))
        def _():
            back_copy.wait_recv()

        @pl.when(edge)
        def _():
            for i in range(2):
                across(relay_buf, 2 * c + i, y_send)[0].wait_recv()

    for copy in flow:
        copy.wait()

    v = [vleft[k] for k in range(4)] + [v_ref[k] for k in range(4)] + [vright[k] for k in range(4)]
    for k in range(10):
        cp[k] = jnp.where(adjoint, diffuse_x + 0.5 * v[k + 2], diffuse_x - 0.5 * v[k + 1])
        cm[k] = jnp.where(adjoint, diffuse_x - 0.5 * v[k], diffuse_x + 0.5 * v[k + 1])

    def sections(snap, base):
        cells = [ref[snap, k].astype(jnp.float32) for ref in (left, u_ref, right) for k in range(4)]
        for section in range(SECTIONS):
            new = []
            for k in range(0, len(cells) - 2, 2):
                pair = jnp.concatenate([cells[k + 1], cells[k + 2]], axis=0).astype(jnp.bfloat16)
                lanes = (pltpu.roll(pair, 1, 1) + pltpu.roll(pair, 127, 1)).astype(jnp.float32)
                for j in range(2):
                    center = cells[k + 1 + j]
                    side = pltpu.roll(center, 1, 0) + pltpu.roll(center, 7, 0) + lanes[8 * j : 8 * j + 8]
                    new.append(
                        keep_center * center
                        + cp[section + k + j] * cells[k + j + 2]
                        + cm[section + k + j] * cells[k + j]
                        + diffuse_side * side
                    )
            cells = new
        for k in range(4):
            stage[pl.ds(base + k * 64, 8, stride=8), :] = cells[k]

    def chain(c):
        return remote(adj_ref.at[c], adj_ref.at[c], a_send.at[c], a_recv.at[c], (lax.max(g - 1, 0), s))

    def relay(c):
        @pl.when(middle)
        def _():
            chain(c).wait_recv()
            chain(c).start()

    def up(c):
        k = lax.min(g, 2)
        return remote(fields.at[k, c], fields.at[k, c], up_send.at[c], d_recv.at[k, c], (lax.min(g + 1, 3), s))

    def down(c):
        k = lax.min(g, 2)
        return remote(fields.at[k, c], fields.at[k, c], down_send.at[c], d_recv.at[k, c], (lax.max(g - 1, 0), s))

    def far(c):
        k = lax.max(lax.min(g - 1, 2), 0)
        return remote(fields.at[k, c], fields.at[k, c], far_send.at[c], d_recv.at[k, c], (lax.min(g + 1, 3), s))

    def chunk(c, carry):
        @pl.when(jnp.logical_not(edge) & (c == lax.div(plane + 2, 4)))
        def _():
            pass_on()

        halo_in(c)

        def one(part_no, inner):
            for i in range(8):
                sections(c * PER + part_no * 8 + i, part_no * 256 + i)
            return inner

        lax.fori_loop(0, 2, one, 0)

        def packed(q):
            low = stage[q * 8 : q * 8 + 8, :]
            high = stage[256 + q * 8 : 256 + q * 8 + 8, :]
            return jnp.concatenate([low, high], axis=0).astype(jnp.bfloat16)

        @pl.when(adjoint)
        def _():
            for q in range(32):
                adj_ref[c, q] = packed(q)
            chain(c).start()

        @pl.when(direct)
        def _():
            for q in range(32):
                fields[lax.min(g, 2), c, q] = packed(q)

            def start_up():
                for i in range(2):
                    up(2 * (c - CHUNKS + 4) + i).start()

            pl.when(c >= CHUNKS - 4)(start_up)

        @pl.when(c >= 1)
        def _():
            relay(c - 1)

        return carry

    lax.fori_loop(0, CHUNKS, chunk, 0)
    relay(CHUNKS - 1)

    def spread_fields(begin, end):
        @pl.when(middle)
        def _():
            def one(c, carry):
                down(c).start()
                far(c).wait_recv()
                far(c).start()
                return carry

            lax.fori_loop(begin, end, one, 0)

    @pl.when(g == 0)
    def _():
        def one(c, carry):
            chain(c).wait_recv()
            return carry

        lax.fori_loop(0, CHUNKS, one, 0)

    spread_fields(0, EARLY)

    def scatter(d):
        p2 = plane_peer(d)
        return remote(part.at[p2], rs_buf.at[plane], p_send.at[p2], p_recv.at[plane], (g, slab_of(zh, p2, core)))

    def scatter_in(d):
        p2 = plane_peer(d)
        return remote(part.at[plane], rs_buf.at[p2], p_send.at[plane], p_recv.at[p2], (g, slab_of(zh, p2, core)))

    slot = g * 4 + zh * 2 + core
    own_slot = lax.min(slot, 11)

    def spread(d):
        return remote(tile, zbuf.at[own_slot], z_send.at[d], z_recv.at[own_slot], peer16(d))

    @pl.when(direct)
    def _():
        here = lax.min(g, 2)

        def product(q, total):
            lhs = [adj_ref[:, 2 * q + j].reshape(SNAP, 128) for j in range(2)]
            rhs = [fields[here, :, 2 * q + j].reshape(SNAP, 128) for j in range(2)]
            return total + lax.dot_general(
                jnp.concatenate(lhs, axis=1),
                jnp.concatenate(rhs, axis=1),
                (((1,), (1,)), ((), ())),
                preferred_element_type=jnp.float32,
            )

        total = lax.fori_loop(0, 16, product, jnp.zeros((SNAP, SNAP), jnp.float32))
        part[...] = total.reshape(16, 8, SNAP)
        for d in range(1, 16):
            scatter(d).start()
        rs_buf[plane] = part[plane]
        for d in range(1, 16):
            scatter_in(d).wait_recv()
        tile[...] = jnp.sum(rs_buf[...], axis=0)
        for d in range(1, 16):
            spread(d).start()
        zbuf[own_slot] = tile[...]

    spread_fields(EARLY, CHUNKS)

    for here in range(12):

        @pl.when(slot != here)
        def _():
            pltpu.make_async_copy(zbuf.at[here], zbuf.at[here], z_recv.at[here]).wait()

    for k in range(3):
        mine[k] = jnp.sum(zbuf[k * 4 : k * 4 + 4], axis=0) * scale

    def share(d):
        p2 = plane_peer(d)
        return remote(mine, coup_ref.at[plane], g_send.at[p2], g_recv.at[plane], (g, slab_of(zh, p2, core)))

    def share_in(d):
        p2 = plane_peer(d)
        return remote(mine, coup_ref.at[p2], g_send.at[plane], g_recv.at[p2], (g, slab_of(zh, p2, core)))

    for d in range(1, 16):
        share(d).start()
    coup_ref[plane] = mine[...]
    for d in range(1, 16):
        share_in(d).wait_recv()

    root = invert(coup_ref, m_ref)

    def weights(row, k):
        return (
            jnp.dot(
                m_ref[pl.ds(pl.multiple_of(row, 32), 32), :],
                coup_ref[:, k].reshape(SNAP, SNAP),
                precision=lax.Precision.HIGHEST,
                preferred_element_type=jnp.float32,
            )
            / root
        ).astype(jnp.bfloat16)

    def times(w, ref, q):
        rhs = jnp.concatenate([ref[:, 2 * q + j].reshape(SNAP, 128) for j in range(2)], axis=1)
        out = jnp.dot(w, rhs, preferred_element_type=jnp.float32)
        return [out[:, j * 128 : j * 128 + 128] for j in range(2)]

    def arrived(k):
        def one(c, carry):
            pltpu.make_async_copy(fields.at[k, c], fields.at[k, c], d_recv.at[k, c]).wait()
            return carry

        lax.fori_loop(0, CHUNKS, one, 0)

    def post(i):
        to = jnp.where(g == 1, 0, 3)
        block = pl.ds(i * 8, 8)
        return remote(terms.at[block], inbox.at[block], t_send.at[i], t_recv.at[i], (to, s))

    for holder, k, row in ((1, 2, 0), (2, 0, 96)):

        @pl.when(g == holder)
        def _():
            arrived(k)
            w = weights(row, k)
            for i in range(4):

                def one(q, carry):
                    for j, x in enumerate(times(w, fields.at[k], q)):
                        terms[2 * q + j] = x.astype(jnp.bfloat16)
                    return carry

                lax.fori_loop(i * 4, i * 4 + 4, one, 0)
                post(i).start()

    own_inverse = m_ref[pl.ds(pl.multiple_of(g * 32, 32), 32), :].astype(jnp.bfloat16)

    def adjoint_modes(q, carry):
        for j, x in enumerate(times(own_inverse, adj_ref, q)):
            am_ref[2 * q + j] = x.astype(jnp.bfloat16)
        return carry

    lax.fori_loop(0, 16, adjoint_modes, 0)

    @pl.when((g == 0) | adjoint)
    def _():
        arrived(1)

    @pl.when(adjoint)
    def _():
        arrived(2)

    w1 = weights(g * 32, 1)

    def one_group(q, carry):
        for j, x in enumerate(times(w1, fields.at[1], q)):
            acc[2 * q + j] = x
        return carry

    lax.fori_loop(0, 16, one_group, 0)
    for k, present in ((0, direct), (2, g > 0)):

        @pl.when(present)
        def _():
            w = weights(g * 32, k)

            def add(q, carry):
                for j, x in enumerate(times(w, fields.at[k], q)):
                    acc[2 * q + j] += x
                return carry

            lax.fori_loop(0, 16, add, 0)

    @pl.when(middle)
    def _():
        def out(q, carry):
            dm_ref[q] = acc[q].astype(jnp.bfloat16)
            return carry

        lax.fori_loop(0, 32, out, 0)

    @pl.when(jnp.logical_not(middle))
    def _():
        for i in range(4):
            block = pl.ds(i * 8, 8)
            pltpu.make_async_copy(inbox.at[block], inbox.at[block], t_recv.at[i]).wait()

            def out(q, carry):
                dm_ref[q] = (acc[q] + inbox[q].astype(jnp.float32)).astype(jnp.bfloat16)
                return carry

            lax.fori_loop(i * 8, i * 8 + 8, out, 0)

    def drain(c, carry):
        ahead_copy, back_copy = halo(c)

        @pl.when(jnp.logical_not(last))
        def _():
            ahead_copy.wait_send()

        @pl.when(jnp.logical_not(first))
        def _():
            back_copy.wait_send()

        @pl.when(g > 0)
        def _():
            chain(c).wait_send()

        @pl.when(direct)
        def _():
            up(c).wait_send()

        @pl.when(middle)
        def _():
            down(c).wait_send()
            far(c).wait_send()

        return carry

    lax.fori_loop(0, CHUNKS, drain, 0)

    @pl.when(edge)
    def _():
        def one(i, carry):
            to_relay(i).wait_send()
            return carry

        lax.fori_loop(0, 16, one, 0)

    @pl.when(jnp.logical_not(edge))
    def _():
        across(relay_buf, plane, y_send)[0].wait_send()

    for d in range(1, 16):
        share(d).wait_send()

    @pl.when(direct)
    def _():
        for d in range(1, 16):
            scatter(d).wait_send()
            spread(d).wait_send()

    @pl.when(middle)
    def _():
        for i in range(4):
            post(i).wait_send()


def invert(coup_ref, m_ref):
    gram = jnp.zeros((SNAP, SNAP), jnp.float32)
    for k in range(3):
        c = coup_ref[:, k].reshape(SNAP, SNAP)
        gram = gram + lax.dot_general(
            c, c, (((1,), (1,)), ((), ())), precision=lax.Precision.HIGHEST, preferred_element_type=jnp.float32
        )
    row = lax.broadcasted_iota(jnp.int32, (SNAP, SNAP), 0)
    col = lax.broadcasted_iota(jnp.int32, (SNAP, SNAP), 1)
    eye = (row == col).astype(jnp.float32)
    energy = jnp.sum(gram * eye, axis=(0, 1), keepdims=True) / SNAP
    m_ref[...] = gram / energy + damping * eye

    sub = lax.broadcasted_iota(jnp.int32, (8, SNAP), 0)
    lane = lax.broadcasted_iota(jnp.int32, (8, SNAP), 1)

    def spread_row(x, j):
        return jnp.broadcast_to(x[j : j + 1, :], (8, SNAP))

    for b in range(16):
        full = m_ref[...]
        columns = [jnp.broadcast_to(full[:, 8 * b + j : 8 * b + j + 1], (SNAP, SNAP)) for j in range(8)]
        panel = full[8 * b : 8 * b + 8, :]
        pivots = [c[8 * b : 8 * b + 8, :] for c in columns]
        for j in range(8):
            own = sub == j
            inv = 1.0 / spread_row(pivots[j], j)
            pj = pivots[j]
            panel = jnp.where(lane == 8 * b + j, own.astype(jnp.float32), panel)
            new = spread_row(panel, j) * inv
            panel = jnp.where(own, new, panel - pj * new)
            for i in range(j + 1, 8):
                new = spread_row(pivots[i], j) * inv
                pivots[i] = jnp.where(own, new, pivots[i] - pj * new)
        inside = (lane >= 8 * b) & (lane < 8 * b + 8)
        spread = [spread_row(panel, j) for j in range(8)]
        for t in range(16):
            if t == b:
                m_ref[8 * t : 8 * t + 8, :] = panel
            else:
                rest = jnp.where(inside, 0.0, full[8 * t : 8 * t + 8, :])
                for j in range(8):
                    rest = rest - columns[j][8 * t : 8 * t + 8, :] * spread[j]
                m_ref[8 * t : 8 * t + 8, :] = rest
    return jnp.sqrt(energy)


def per_device(snapshots, base_flow):
    field = snapshots[0]
    f32, bf16 = jnp.float32, jnp.bfloat16
    vmem = pl.BlockSpec(memory_space=pltpu.VMEM)
    dma = pltpu.SemaphoreType.DMA
    slab_shape = field.shape
    cells = 64 * math.prod(slab_shape[1:])
    scale = 1.0 / math.sqrt(cells)
    modes = jax.ShapeDtypeStruct((32, 32, 128), bf16)
    dm, am = pl.pallas_call(
        functools.partial(kernel, scale),
        out_shape=(modes, modes),
        in_specs=[vmem] * 2,
        out_specs=(vmem,) * 2,
        scratch_shapes=[
            pltpu.VMEM(slab_shape, bf16),
            pltpu.VMEM(slab_shape, bf16),
            pltpu.VMEM((8,) + slab_shape[1:], bf16),
            pltpu.VMEM((4, 8, 128), f32),
            pltpu.VMEM((4, 8, 128), f32),
            pltpu.VMEM((10, 8, 128), f32),
            pltpu.VMEM((10, 8, 128), f32),
            pltpu.VMEM((512, 128), f32),
            pltpu.VMEM((3, CHUNKS, 32, PER, 128), bf16),
            pltpu.VMEM((CHUNKS, 32, PER, 128), bf16),
            pltpu.VMEM((16, 8, SNAP), f32),
            pltpu.VMEM((16, 8, SNAP), f32),
            pltpu.VMEM((8, SNAP), f32),
            pltpu.VMEM((12, 8, SNAP), f32),
            pltpu.VMEM((3, 8, SNAP), f32),
            pltpu.VMEM((16, 3, 8, SNAP), f32),
            pltpu.VMEM((SNAP, SNAP), f32),
            pltpu.VMEM((32, 32, 128), f32),
            pltpu.VMEM((32, 32, 128), bf16),
            pltpu.VMEM((32, 32, 128), bf16),
            dma((2, CHUNKS)),
            dma((2, CHUNKS)),
            dma((2,)),
            dma((2,)),
            dma((16,)),
            dma((16,)),
            dma,
            dma,
            dma((CHUNKS,)),
            dma((CHUNKS,)),
            dma((CHUNKS,)),
            dma((CHUNKS,)),
            dma((CHUNKS,)),
            dma((3, CHUNKS)),
            dma((16,)),
            dma((16,)),
            dma((16,)),
            dma((12,)),
            dma((16,)),
            dma((16,)),
            dma((4,)),
            dma((4,)),
        ],
        compiler_params=pltpu.CompilerParams(
            collective_id=0, has_side_effects=True, vmem_limit_bytes=48 * MIB
        ),
        name="pod",
    )(field, base_flow)

    def placed(x):
        return x.reshape(4, 8, 32, 128).transpose(2, 0, 1, 3)

    return placed(dm), placed(am)


def solution(mesh):
    return jax.shard_map(
        per_device,
        mesh=mesh,
        in_specs=(P("grp", None, "slab", None, None), P("slab", None, None)),
        out_specs=(P("grp", "slab", None, None), P("grp", "slab", None, None)),
        check_vma=False,
    )
```

```python
import functools
import math

import jax
import jax.numpy as jnp
from jax import lax
from jax.experimental import pallas as pl
from jax.experimental.pallas import tpu as pltpu
from jax.sharding import PartitionSpec as P

SNAP = 128
SECTIONS = 4
CHUNKS = 8
PER = SNAP // CHUNKS
MESH = pl.DeviceIdType.MESH
MIB = 1 << 20

diffuse_x = 0.35
diffuse_side = 0.05
keep_center = 0.1
damping = 0.5


def remote(src, dst, send_sem, recv_sem, device):
    return pltpu.make_async_remote_copy(
        src_ref=src, dst_ref=dst, send_sem=send_sem, recv_sem=recv_sem, device_id=device, device_id_type=MESH
    )


def place():
    g = lax.axis_index("grp")
    s = lax.axis_index("slab")
    core = lax.rem(s, 2)
    plane = lax.rem(lax.div(s, 2), 16)
    zh = lax.div(s, 32)
    return g, s, core, plane, zh


def slab_of(zh, plane, core):
    return zh * 32 + plane * 2 + core


def kernel(
    scale,
    u_ref,
    v_ref,
    dm_ref,
    am_ref,
    left,
    right,
    relay_buf,
    vleft,
    vright,
    cp,
    cm,
    stage,
    own,
    quart,
    part,
    rs_buf,
    tile,
    zbuf,
    mine,
    coup_ref,
    m_ref,
    wide,
    terms,
    h_send,
    h_recv,
    v_send,
    v_recv,
    x_send,
    x_recv,
    y_send,
    y_recv,
    q_send,
    q_recv,
    p_send,
    p_recv,
    z_send,
    z_recv,
    g_send,
    g_recv,
    o_send,
    o_recv,
):
    g, s, core, plane, zh = place()
    ahead = lax.rem(s + 1, 64)
    back = lax.rem(s + 63, 64)
    adjoint = g == 3
    z = zh * 4 + g
    last = (plane == 15) & (core == 1)
    first = (plane == 0) & (core == 0)
    edge = last | first

    def at(depth, position, side):
        depth = lax.rem(depth, 8)
        return lax.rem(depth, 4), slab_of(lax.div(depth, 4), position, side)

    def peer16(d):
        g2 = lax.rem(g + d // 4, 4)
        zh2 = lax.rem(zh + (d // 2) % 2, 2)
        c2 = lax.rem(core + d % 2, 2)
        return g2, slab_of(zh2, plane, c2)

    def plane_peer(d):
        return lax.rem(plane + d, 16)

    barrier = pltpu.get_barrier_semaphore()

    def greet(device):
        pl.semaphore_signal(barrier, inc=1, device_id=device, device_id_type=MESH)

    greet((g, ahead))
    greet((g, back))
    for d in range(1, 16):
        greet((g, slab_of(zh, plane_peer(d), core)))
        greet(peer16(d))

    far_end = at(z + 4, 15 * (1 - core), 1 - core)
    greet(far_end)

    @pl.when(edge)
    def _():
        def one(i, carry):
            greet(at(z + 4, i, 1 - core))
            return carry

        lax.fori_loop(0, 16, one, 0)

    pl.semaphore_wait(barrier, 33 + jnp.where(edge, 16, 0))

    flow = [
        remote(v_ref, vleft, v_send.at[0], v_recv.at[0], (g, ahead)),
        remote(v_ref, vright, v_send.at[1], v_recv.at[1], (g, back)),
    ]
    for copy in flow:
        copy.start()

    def rows(c):
        return pl.ds(c * PER, PER)

    def halo(c):
        return [
            remote(u_ref.at[rows(c)], left.at[rows(c)], h_send.at[0, c], h_recv.at[0, c], (g, ahead)),
            remote(u_ref.at[rows(c)], right.at[rows(c)], h_send.at[1, c], h_recv.at[1, c], (g, back)),
        ]

    def half(i):
        return pl.ds(i * 8, 8)

    def to_relay(i):
        return remote(u_ref.at[half(i)], relay_buf, x_send.at[i], y_recv, (g, slab_of(zh, i, core)))

    def across(src, i, send_sem):
        return (
            remote(src, right.at[half(i)], send_sem, x_recv.at[i], far_end),
            remote(src, left.at[half(i)], send_sem, x_recv.at[i], far_end),
        )

    def start_across(src, i, send_sem):
        to_right, to_left = across(src, i, send_sem)

        @pl.when(core == 0)
        def _():
            to_right.start()

        @pl.when(core == 1)
        def _():
            to_left.start()

    @pl.when(edge)
    def _():
        def one(i, carry):
            @pl.when(i != plane)
            def _():
                to_relay(i).start()

            @pl.when(i == plane)
            def _():
                start_across(u_ref.at[half(i)], i, x_send.at[i])

            return carry

        lax.fori_loop(0, 16, one, 0)

    def start_halo(c, carry):
        ahead_copy, back_copy = halo(c)

        @pl.when(jnp.logical_not(last))
        def _():
            ahead_copy.start()

        @pl.when(jnp.logical_not(first))
        def _():
            back_copy.start()

        return carry

    lax.fori_loop(0, CHUNKS, start_halo, 0)

    def pass_on():
        pltpu.make_async_copy(relay_buf, relay_buf, y_recv).wait()
        start_across(relay_buf, plane, y_send)

    def halo_in(c):
        ahead_copy, back_copy = halo(c)

        @pl.when(jnp.logical_not(first))
        def _():
            ahead_copy.wait_recv()

        @pl.when(jnp.logical_not(last))
        def _():
            back_copy.wait_recv()

        @pl.when(edge)
        def _():
            for i in range(2):
                across(relay_buf, 2 * c + i, y_send)[0].wait_recv()

    for copy in flow:
        copy.wait()

    v = [vleft[k] for k in range(4)] + [v_ref[k] for k in range(4)] + [vright[k] for k in range(4)]
    for k in range(10):
        cp[k] = jnp.where(adjoint, diffuse_x + 0.5 * v[k + 2], diffuse_x - 0.5 * v[k + 1])
        cm[k] = jnp.where(adjoint, diffuse_x - 0.5 * v[k], diffuse_x + 0.5 * v[k + 1])

    def sections(snap, base):
        cells = [ref[snap, k].astype(jnp.float32) for ref in (left, u_ref, right) for k in range(4)]
        for section in range(SECTIONS):
            new = []
            for k in range(0, len(cells) - 2, 2):
                pair = jnp.concatenate([cells[k + 1], cells[k + 2]], axis=0).astype(jnp.bfloat16)
                lanes = (pltpu.roll(pair, 1, 1) + pltpu.roll(pair, 127, 1)).astype(jnp.float32)
                for j in range(2):
                    center = cells[k + 1 + j]
                    side = pltpu.roll(center, 1, 0) + pltpu.roll(center, 7, 0) + lanes[8 * j : 8 * j + 8]
                    new.append(
                        keep_center * center
                        + cp[section + k + j] * cells[k + j + 2]
                        + cm[section + k + j] * cells[k + j]
                        + diffuse_side * side
                    )
            cells = new
        for k in range(4):
            stage[pl.ds(base + k * 64, 8, stride=8), :] = cells[k]

    def piece(c, d):
        r = lax.rem(g + d, 4)
        return remote(own.at[c, r], quart.at[g, c], q_send.at[c, d], q_recv.at[g, c], (r, s))

    def piece_in(c, d):
        k = lax.rem(g + d, 4)
        return remote(own.at[c, k], quart.at[k, c], q_send.at[c, d], q_recv.at[k, c], (k, s))

    def chunk(c, carry):
        @pl.when(jnp.logical_not(edge) & (c == lax.div(plane + 2, 5)))
        def _():
            pass_on()

        halo_in(c)

        def one(part_no, inner):
            for i in range(8):
                sections(c * PER + part_no * 8 + i, part_no * 256 + i)
            return inner

        lax.fori_loop(0, 2, one, 0)

        def packed(q):
            low = stage[q * 8 : q * 8 + 8, :]
            high = stage[256 + q * 8 : 256 + q * 8 + 8, :]
            return jnp.concatenate([low, high], axis=0).astype(jnp.bfloat16)

        for q in range(32):
            own[c, q // 8, q % 8] = packed(q)
        for d in range(1, 4):
            piece(c, d).start()
        quart[g, c] = own[c, g]
        return carry

    lax.fori_loop(0, CHUNKS, chunk, 0)

    def gathered(c, carry):
        for d in range(1, 4):
            piece_in(c, d).wait_recv()
        return carry

    lax.fori_loop(0, CHUNKS, gathered, 0)

    def scatter(d):
        p2 = plane_peer(d)
        return remote(part.at[p2], rs_buf.at[plane], p_send.at[p2], p_recv.at[plane], (g, slab_of(zh, p2, core)))

    def scatter_in(d):
        p2 = plane_peer(d)
        return remote(part.at[plane], rs_buf.at[p2], p_send.at[plane], p_recv.at[p2], (g, slab_of(zh, p2, core)))

    slot = g * 4 + zh * 2 + core

    def spread(d):
        return remote(tile, zbuf.at[slot], z_send.at[d], z_recv.at[slot], peer16(d))

    def pair(k, q):
        return jnp.concatenate([quart[k, :, 2 * q + j].reshape(SNAP, 128) for j in range(2)], axis=1)

    for k in range(3):

        def product(q, total):
            return total + lax.dot_general(
                pair(3, q), pair(k, q), (((1,), (1,)), ((), ())), preferred_element_type=jnp.float32
            )

        total = lax.fori_loop(0, 4, product, jnp.zeros((SNAP, SNAP), jnp.float32))
        part[:, k] = total.reshape(16, 8, SNAP)
    for d in range(1, 16):
        scatter(d).start()
    rs_buf[plane] = part[plane]
    for d in range(1, 16):
        scatter_in(d).wait_recv()
    tile[...] = jnp.sum(rs_buf[...], axis=0)
    for d in range(1, 16):
        spread(d).start()
    zbuf[slot] = tile[...]
    for here in range(16):

        @pl.when(slot != here)
        def _():
            pltpu.make_async_copy(zbuf.at[here], zbuf.at[here], z_recv.at[here]).wait()

    mine[...] = jnp.sum(zbuf[...], axis=0) * scale

    def share(d):
        p2 = plane_peer(d)
        return remote(mine, coup_ref.at[plane], g_send.at[p2], g_recv.at[plane], (g, slab_of(zh, p2, core)))

    def share_in(d):
        p2 = plane_peer(d)
        return remote(mine, coup_ref.at[p2], g_send.at[plane], g_recv.at[p2], (g, slab_of(zh, p2, core)))

    for d in range(1, 16):
        share(d).start()
    coup_ref[plane] = mine[...]
    for d in range(1, 16):
        share_in(d).wait_recv()

    root = invert(coup_ref, m_ref)

    def post(d, kind):
        r = lax.rem(g + d, 4)
        out = (dm_ref, am_ref)[kind]
        here = pl.ds(pl.multiple_of(g * 8, 8), 8)
        return remote(terms.at[kind, r], out.at[here], o_send.at[kind, d], o_recv.at[kind, g], (r, s))

    def post_in(d, kind):
        k = lax.rem(g + d, 4)
        out = (dm_ref, am_ref)[kind]
        there = pl.ds(pl.multiple_of(k * 8, 8), 8)
        return remote(terms.at[kind, k], out.at[there], o_send.at[kind, d], o_recv.at[kind, k], (k, s))

    def modes(kind, value):
        def one(q, carry):
            x = value(q).astype(jnp.bfloat16)
            for j in range(2):
                terms[kind, :, 2 * q + j] = x[:, j * 128 : j * 128 + 128].reshape(4, 32, 128)
            return carry

        lax.fori_loop(0, 4, one, 0)
        for d in (2, 3, 1):
            post(d, kind).start()
        here = pl.ds(pl.multiple_of(g * 8, 8), 8)
        (dm_ref, am_ref)[kind][here] = terms[kind, g]

    inverse = m_ref[...].astype(jnp.bfloat16)
    modes(1, lambda q: jnp.dot(inverse, pair(3, q), preferred_element_type=jnp.float32))
    for k in range(3):
        wide[k] = (
            jnp.dot(
                m_ref[...],
                coup_ref[:, k].reshape(SNAP, SNAP),
                precision=lax.Precision.HIGHEST,
                preferred_element_type=jnp.float32,
            )
            / root
        ).astype(jnp.bfloat16)

    def direct_value(q):
        total = jnp.dot(wide[0], pair(0, q), preferred_element_type=jnp.float32)
        for k in (1, 2):
            total = total + jnp.dot(wide[k], pair(k, q), preferred_element_type=jnp.float32)
        return total

    modes(0, direct_value)
    for kind in (1, 0):
        for d in range(1, 4):
            post_in(d, kind).wait_recv()

    def drain(c, carry):
        ahead_copy, back_copy = halo(c)

        @pl.when(jnp.logical_not(last))
        def _():
            ahead_copy.wait_send()

        @pl.when(jnp.logical_not(first))
        def _():
            back_copy.wait_send()

        for d in range(1, 4):
            piece(c, d).wait_send()
        return carry

    lax.fori_loop(0, CHUNKS, drain, 0)

    @pl.when(edge)
    def _():
        def one(i, carry):
            to_relay(i).wait_send()
            return carry

        lax.fori_loop(0, 16, one, 0)

    @pl.when(jnp.logical_not(edge))
    def _():
        across(relay_buf, plane, y_send)[0].wait_send()

    for d in range(1, 16):
        scatter(d).wait_send()
        spread(d).wait_send()
        share(d).wait_send()
    for kind in range(2):
        for d in range(1, 4):
            post(d, kind).wait_send()


def invert(coup_ref, m_ref):
    gram = jnp.zeros((SNAP, SNAP), jnp.float32)
    for k in range(3):
        c = coup_ref[:, k].reshape(SNAP, SNAP)
        gram = gram + lax.dot_general(
            c, c, (((1,), (1,)), ((), ())), precision=lax.Precision.HIGHEST, preferred_element_type=jnp.float32
        )
    row = lax.broadcasted_iota(jnp.int32, (SNAP, SNAP), 0)
    col = lax.broadcasted_iota(jnp.int32, (SNAP, SNAP), 1)
    eye = (row == col).astype(jnp.float32)
    energy = jnp.sum(gram * eye, axis=(0, 1), keepdims=True) / SNAP
    m_ref[...] = gram / energy + damping * eye

    sub = lax.broadcasted_iota(jnp.int32, (8, SNAP), 0)
    lane = lax.broadcasted_iota(jnp.int32, (8, SNAP), 1)

    def spread_row(x, j):
        return jnp.broadcast_to(x[j : j + 1, :], (8, SNAP))

    for b in range(16):
        full = m_ref[...]
        columns = [jnp.broadcast_to(full[:, 8 * b + j : 8 * b + j + 1], (SNAP, SNAP)) for j in range(8)]
        panel = full[8 * b : 8 * b + 8, :]
        pivots = [c[8 * b : 8 * b + 8, :] for c in columns]
        for j in range(8):
            own = sub == j
            inv = 1.0 / spread_row(pivots[j], j)
            pj = pivots[j]
            panel = jnp.where(lane == 8 * b + j, own.astype(jnp.float32), panel)
            new = spread_row(panel, j) * inv
            panel = jnp.where(own, new, panel - pj * new)
            for i in range(j + 1, 8):
                new = spread_row(pivots[i], j) * inv
                pivots[i] = jnp.where(own, new, pivots[i] - pj * new)
        inside = (lane >= 8 * b) & (lane < 8 * b + 8)
        spread = [spread_row(panel, j) for j in range(8)]
        for t in range(16):
            if t == b:
                m_ref[8 * t : 8 * t + 8, :] = panel
            else:
                rest = jnp.where(inside, 0.0, full[8 * t : 8 * t + 8, :])
                for j in range(8):
                    rest = rest - columns[j][8 * t : 8 * t + 8, :] * spread[j]
                m_ref[8 * t : 8 * t + 8, :] = rest
    return jnp.sqrt(energy)


def per_device(snapshots, base_flow):
    field = snapshots[0]
    f32, bf16 = jnp.float32, jnp.bfloat16
    vmem = pl.BlockSpec(memory_space=pltpu.VMEM)
    dma = pltpu.SemaphoreType.DMA
    slab_shape = field.shape
    cells = 64 * math.prod(slab_shape[1:])
    scale = 1.0 / math.sqrt(cells)
    modes = jax.ShapeDtypeStruct((32, 32, 128), bf16)
    dm, am = pl.pallas_call(
        functools.partial(kernel, scale),
        out_shape=(modes, modes),
        in_specs=[vmem] * 2,
        out_specs=(vmem,) * 2,
        scratch_shapes=[
            pltpu.VMEM(slab_shape, bf16),
            pltpu.VMEM(slab_shape, bf16),
            pltpu.VMEM((8,) + slab_shape[1:], bf16),
            pltpu.VMEM((4, 8, 128), f32),
            pltpu.VMEM((4, 8, 128), f32),
            pltpu.VMEM((10, 8, 128), f32),
            pltpu.VMEM((10, 8, 128), f32),
            pltpu.VMEM((512, 128), f32),
            pltpu.VMEM((CHUNKS, 4, 8, PER, 128), bf16),
            pltpu.VMEM((4, CHUNKS, 8, PER, 128), bf16),
            pltpu.VMEM((16, 3, 8, SNAP), f32),
            pltpu.VMEM((16, 3, 8, SNAP), f32),
            pltpu.VMEM((3, 8, SNAP), f32),
            pltpu.VMEM((16, 3, 8, SNAP), f32),
            pltpu.VMEM((3, 8, SNAP), f32),
            pltpu.VMEM((16, 3, 8, SNAP), f32),
            pltpu.VMEM((SNAP, SNAP), f32),
            pltpu.VMEM((3, SNAP, SNAP), bf16),
            pltpu.VMEM((2, 4, 8, 32, 128), bf16),
            dma((2, CHUNKS)),
            dma((2, CHUNKS)),
            dma((2,)),
            dma((2,)),
            dma((16,)),
            dma((16,)),
            dma,
            dma,
            dma((CHUNKS, 4)),
            dma((4, CHUNKS)),
            dma((16,)),
            dma((16,)),
            dma((16,)),
            dma((16,)),
            dma((16,)),
            dma((16,)),
            dma((2, 4)),
            dma((2, 4)),
        ],
        compiler_params=pltpu.CompilerParams(
            collective_id=0, has_side_effects=True, vmem_limit_bytes=48 * MIB
        ),
        name="pod",
    )(field, base_flow)

    def placed(x):
        return x.reshape(4, 8, 32, 128).transpose(2, 0, 1, 3)

    return placed(dm), placed(am)


def solution(mesh):
    return jax.shard_map(
        per_device,
        mesh=mesh,
        in_specs=(P("grp", None, "slab", None, None), P("slab", None, None)),
        out_specs=(P("grp", "slab", None, None), P("grp", "slab", None, None)),
        check_vma=False,
    )
```

```python
import functools
import math

import jax
import jax.numpy as jnp
from jax import lax
from jax.experimental import pallas as pl
from jax.experimental.pallas import tpu as pltpu
from jax.sharding import PartitionSpec as P

SNAP = 128
SECTIONS = 4
CHUNKS = 8
PER = SNAP // CHUNKS
MESH = pl.DeviceIdType.MESH
MIB = 1 << 20

diffuse_x = 0.35
diffuse_side = 0.05
keep_center = 0.1
damping = 0.5


def remote(src, dst, send_sem, recv_sem, device):
    return pltpu.make_async_remote_copy(
        src_ref=src, dst_ref=dst, send_sem=send_sem, recv_sem=recv_sem, device_id=device, device_id_type=MESH
    )


def place():
    g = lax.axis_index("grp")
    s = lax.axis_index("slab")
    core = lax.rem(s, 2)
    plane = lax.rem(lax.div(s, 2), 16)
    zh = lax.div(s, 32)
    return g, s, core, plane, zh


def slab_of(zh, plane, core):
    return zh * 32 + plane * 2 + core


def kernel(
    scale,
    u_hbm,
    v_hbm,
    dm_ref,
    am_ref,
    u_ref,
    v_ref,
    left,
    right,
    relay_buf,
    vleft,
    vright,
    cp,
    cm,
    stage,
    own,
    quart,
    part,
    pair_buf,
    rs_buf,
    tile,
    zbuf,
    mine,
    coup_ref,
    m_ref,
    wide,
    terms,
    in_sem,
    c_send,
    c_recv,
    h_send,
    h_recv,
    v_send,
    v_recv,
    x_send,
    x_recv,
    y_send,
    y_recv,
    q_send,
    q_recv,
    p_send,
    p_recv,
    z_send,
    z_recv,
    g_send,
    g_recv,
    o_send,
    o_recv,
):
    g, s, core, plane, zh = place()
    ahead = lax.rem(s + 1, 64)
    back = lax.rem(s + 63, 64)
    adjoint = g == 3
    z = zh * 4 + g
    last = (plane == 15) & (core == 1)
    first = (plane == 0) & (core == 0)
    edge = last | first

    def at(depth, position, side):
        depth = lax.rem(depth, 8)
        return lax.rem(depth, 4), slab_of(lax.div(depth, 4), position, side)

    def plane_peer(d):
        return lax.rem(plane + d, 16)

    owner = lax.div(plane, 8) == core
    partner = (g, slab_of(zh, plane, 1 - core))
    loads = [
        pltpu.make_async_copy(v_hbm, v_ref, in_sem.at[0]),
        pltpu.make_async_copy(u_hbm, u_ref, in_sem.at[1]),
    ]
    for load in loads:
        load.start()
    barrier = pltpu.get_barrier_semaphore()

    def greet(device):
        pl.semaphore_signal(barrier, inc=1, device_id=device, device_id_type=MESH)

    greet((g, ahead))
    greet((g, back))
    greet(partner)
    for d in range(1, 16):
        for side in (core, 1 - core):
            greet((g, slab_of(zh, plane_peer(d), side)))
    for d in range(1, 8):
        greet(at(z + d, plane, core))
    far_end = at(z + 4, 15 * (1 - core), 1 - core)
    greet(far_end)

    @pl.when(edge)
    def _():
        def one(i, carry):
            greet(at(z + 4, i, 1 - core))
            return carry

        lax.fori_loop(0, 16, one, 0)

    for load in loads:
        load.wait()
    pl.semaphore_wait(barrier, 41 + jnp.where(edge, 16, 0))

    flow = [
        remote(v_ref, vleft, v_send.at[0], v_recv.at[0], (g, ahead)),
        remote(v_ref, vright, v_send.at[1], v_recv.at[1], (g, back)),
    ]
    for copy in flow:
        copy.start()

    def rows(c):
        return pl.ds(c * PER, PER)

    def halo(c):
        return [
            remote(u_ref.at[rows(c)], left.at[rows(c)], h_send.at[0, c], h_recv.at[0, c], (g, ahead)),
            remote(u_ref.at[rows(c)], right.at[rows(c)], h_send.at[1, c], h_recv.at[1, c], (g, back)),
        ]

    def half(i):
        return pl.ds(i * 8, 8)

    def to_relay(i):
        return remote(u_ref.at[half(i)], relay_buf, x_send.at[i], y_recv, (g, slab_of(zh, i, core)))

    def across(src, i, send_sem):
        return (
            remote(src, right.at[half(i)], send_sem, x_recv.at[i], far_end),
            remote(src, left.at[half(i)], send_sem, x_recv.at[i], far_end),
        )

    def start_across(src, i, send_sem):
        to_right, to_left = across(src, i, send_sem)

        @pl.when(core == 0)
        def _():
            to_right.start()

        @pl.when(core == 1)
        def _():
            to_left.start()

    @pl.when(edge)
    def _():
        def one(i, carry):
            @pl.when(i != plane)
            def _():
                to_relay(i).start()

            @pl.when(i == plane)
            def _():
                start_across(u_ref.at[half(i)], i, x_send.at[i])

            return carry

        lax.fori_loop(0, 16, one, 0)

    def start_halo(c, carry):
        ahead_copy, back_copy = halo(c)

        @pl.when(jnp.logical_not(last))
        def _():
            ahead_copy.start()

        @pl.when(jnp.logical_not(first))
        def _():
            back_copy.start()

        return carry

    lax.fori_loop(0, CHUNKS, start_halo, 0)

    def pass_on():
        pltpu.make_async_copy(relay_buf, relay_buf, y_recv).wait()
        start_across(relay_buf, plane, y_send)

    def halo_in(c):
        ahead_copy, back_copy = halo(c)

        @pl.when(jnp.logical_not(first))
        def _():
            ahead_copy.wait_recv()

        @pl.when(jnp.logical_not(last))
        def _():
            back_copy.wait_recv()

        @pl.when(edge)
        def _():
            for i in range(2):
                across(relay_buf, 2 * c + i, y_send)[0].wait_recv()

    for copy in flow:
        copy.wait()

    v = [vleft[k] for k in range(4)] + [v_ref[k] for k in range(4)] + [vright[k] for k in range(4)]
    for k in range(10):
        cp[k] = jnp.where(adjoint, diffuse_x + 0.5 * v[k + 2], diffuse_x - 0.5 * v[k + 1])
        cm[k] = jnp.where(adjoint, diffuse_x - 0.5 * v[k], diffuse_x + 0.5 * v[k + 1])

    def sections(snap, base):
        cells = [ref[snap, k].astype(jnp.float32) for ref in (left, u_ref, right) for k in range(4)]
        for section in range(SECTIONS):
            new = []
            for k in range(0, len(cells) - 2, 2):
                pair = jnp.concatenate([cells[k + 1], cells[k + 2]], axis=0).astype(jnp.bfloat16)
                lanes = (pltpu.roll(pair, 1, 1) + pltpu.roll(pair, 127, 1)).astype(jnp.float32)
                for j in range(2):
                    center = cells[k + 1 + j]
                    side = pltpu.roll(center, 1, 0) + pltpu.roll(center, 7, 0) + lanes[8 * j : 8 * j + 8]
                    new.append(
                        keep_center * center
                        + cp[section + k + j] * cells[k + j + 2]
                        + cm[section + k + j] * cells[k + j]
                        + diffuse_side * side
                    )
            cells = new
        for k in range(4):
            stage[pl.ds(base + k * 64, 8, stride=8), :] = cells[k]

    def piece(c, d):
        r = lax.rem(g + d, 4)
        return remote(own.at[c, r], quart.at[g, c], q_send.at[c, d], q_recv.at[g, c], (r, s))

    def piece_in(c, d):
        k = lax.rem(g + d, 4)
        return remote(own.at[c, k], quart.at[k, c], q_send.at[c, d], q_recv.at[k, c], (k, s))

    def chunk(c, carry):
        @pl.when(jnp.logical_not(edge) & (c == lax.div(plane + 2, 5)))
        def _():
            pass_on()

        halo_in(c)

        def one(part_no, inner):
            for i in range(8):
                sections(c * PER + part_no * 8 + i, part_no * 256 + i)
            return inner

        lax.fori_loop(0, 2, one, 0)

        def packed(q):
            low = stage[q * 8 : q * 8 + 8, :]
            high = stage[256 + q * 8 : 256 + q * 8 + 8, :]
            return jnp.concatenate([low, high], axis=0).astype(jnp.bfloat16)

        for q in range(32):
            own[c, q // 8, q % 8] = packed(q)
        for d in range(1, 4):
            piece(c, d).start()
        quart[g, c] = own[c, g]
        return carry

    lax.fori_loop(0, CHUNKS, chunk, 0)

    def gathered(c, carry):
        for d in range(1, 4):
            piece_in(c, d).wait_recv()
        return carry

    lax.fori_loop(0, CHUNKS, gathered, 0)

    def plane_device(p2, side):
        return g, slab_of(zh, p2, side)

    def swap():
        return remote(part.at[pl.ds((1 - core) * 8, 8)], pair_buf, c_send, c_recv, partner)

    def scatter(i):
        p2 = core * 8 + i
        return remote(part.at[p2], rs_buf.at[plane], p_send.at[i], p_recv.at[plane], plane_device(p2, core))

    def spread(d):
        return remote(tile, zbuf.at[z], z_send.at[d], z_recv.at[z], at(z + d, plane, core))

    def share(d, side):
        p2 = plane_peer(d)
        return remote(mine, coup_ref.at[plane], g_send.at[side, d], g_recv.at[plane], plane_device(p2, lax.rem(core + side, 2)))

    def landed(ref, sem, i, skip):
        @pl.when(jnp.logical_not(skip))
        def _():
            pltpu.make_async_copy(ref.at[i], ref.at[i], sem.at[i]).wait()

    def hops(d):
        return min(d // 4, 4 - d // 4) + min(d % 4, 4 - d % 4)

    others = [(d, side) for side in range(2) for d in range(16) if d or side]
    others.sort(key=lambda pair: -hops(pair[0]))

    def pair(k, q):
        return jnp.concatenate([quart[k, :, 2 * q + j].reshape(SNAP, 128) for j in range(2)], axis=1)

    def product(q, totals):
        lhs = pair(3, q)
        wide_two = jnp.concatenate([pair(0, q), pair(1, q)], axis=0)

        def against(rhs):
            return lax.dot_general(lhs, rhs, (((1,), (1,)), ((), ())), preferred_element_type=jnp.float32)

        return totals[0] + against(wide_two), totals[1] + against(pair(2, q))

    two, one_more = lax.fori_loop(
        0, 4, product, (jnp.zeros((SNAP, 2 * SNAP), jnp.float32), jnp.zeros((SNAP, SNAP), jnp.float32))
    )
    for k, total in enumerate((two[:, :SNAP], two[:, SNAP:], one_more)):
        part[:, k] = total.reshape(16, 8, SNAP)
    swap().start()
    swap().wait_recv()
    for i in range(8):
        p2 = core * 8 + i
        part[p2] += pair_buf[i]

        @pl.when(p2 != plane)
        def _():
            scatter(i).start()

    @pl.when(owner)
    def _():
        rs_buf[plane] = part[plane]
        for i in range(16):
            landed(rs_buf, p_recv, i, plane == i)
        tile[...] = jnp.sum(rs_buf[...], axis=0)
        for d in range(1, 8):
            spread(d).start()
        zbuf[z] = tile[...]
        for i in range(8):
            landed(zbuf, z_recv, i, z == i)
        mine[...] = jnp.sum(zbuf[...], axis=0) * scale
        for d, side in others:
            share(d, side).start()
        coup_ref[plane] = mine[...]

    for i in range(16):
        landed(coup_ref, g_recv, i, owner & (plane == i))

    root = invert(coup_ref, m_ref)

    def post(d, kind):
        r = lax.rem(g + d, 4)
        out = (dm_ref, am_ref)[kind]
        here = pl.ds(pl.multiple_of(g * 8, 8), 8)
        return remote(terms.at[kind, r], out.at[here], o_send.at[kind, d], o_recv.at[kind, g], (r, s))

    def post_in(d, kind):
        k = lax.rem(g + d, 4)
        out = (dm_ref, am_ref)[kind]
        there = pl.ds(pl.multiple_of(k * 8, 8), 8)
        return remote(terms.at[kind, k], out.at[there], o_send.at[kind, d], o_recv.at[kind, k], (k, s))

    def modes(kind, value):
        def one(q, carry):
            x = value(q).astype(jnp.bfloat16)
            for j in range(2):
                terms[kind, :, 2 * q + j] = x[:, j * 128 : j * 128 + 128].reshape(4, 32, 128)
            return carry

        lax.fori_loop(0, 4, one, 0)
        for d in (2, 3, 1):
            post(d, kind).start()
        here = pl.ds(pl.multiple_of(g * 8, 8), 8)
        (dm_ref, am_ref)[kind][here] = terms[kind, g]

    inverse = m_ref[...].astype(jnp.bfloat16)
    modes(1, lambda q: jnp.dot(inverse, pair(3, q), preferred_element_type=jnp.float32))
    for k in range(3):
        wide[k] = (
            jnp.dot(
                m_ref[...],
                coup_ref[:, k].reshape(SNAP, SNAP),
                precision=lax.Precision.HIGHEST,
                preferred_element_type=jnp.float32,
            )
            / root
        ).astype(jnp.bfloat16)

    def direct_value(q):
        total = jnp.dot(wide[0], pair(0, q), preferred_element_type=jnp.float32)
        for k in (1, 2):
            total = total + jnp.dot(wide[k], pair(k, q), preferred_element_type=jnp.float32)
        return total

    modes(0, direct_value)
    for kind in (1, 0):
        for d in range(1, 4):
            post_in(d, kind).wait_recv()

    def drain(c, carry):
        ahead_copy, back_copy = halo(c)

        @pl.when(jnp.logical_not(last))
        def _():
            ahead_copy.wait_send()

        @pl.when(jnp.logical_not(first))
        def _():
            back_copy.wait_send()

        for d in range(1, 4):
            piece(c, d).wait_send()
        return carry

    lax.fori_loop(0, CHUNKS, drain, 0)

    @pl.when(edge)
    def _():
        def one(i, carry):
            to_relay(i).wait_send()
            return carry

        lax.fori_loop(0, 16, one, 0)

    @pl.when(jnp.logical_not(edge))
    def _():
        across(relay_buf, plane, y_send)[0].wait_send()

    swap().wait_send()
    for i in range(8):

        @pl.when(core * 8 + i != plane)
        def _():
            scatter(i).wait_send()

    @pl.when(owner)
    def _():
        for d in range(1, 8):
            spread(d).wait_send()
        for d, side in others:
            share(d, side).wait_send()

    for kind in range(2):
        for d in range(1, 4):
            post(d, kind).wait_send()


def invert(coup_ref, m_ref):
    gram = jnp.zeros((SNAP, SNAP), jnp.float32)
    for k in range(3):
        c = coup_ref[:, k].reshape(SNAP, SNAP)
        gram = gram + lax.dot_general(
            c, c, (((1,), (1,)), ((), ())), precision=lax.Precision.HIGHEST, preferred_element_type=jnp.float32
        )
    row = lax.broadcasted_iota(jnp.int32, (SNAP, SNAP), 0)
    col = lax.broadcasted_iota(jnp.int32, (SNAP, SNAP), 1)
    eye = (row == col).astype(jnp.float32)
    energy = jnp.sum(gram * eye, axis=(0, 1), keepdims=True) / SNAP
    m_ref[...] = gram / energy + damping * eye

    sub = lax.broadcasted_iota(jnp.int32, (8, SNAP), 0)
    lane = lax.broadcasted_iota(jnp.int32, (8, SNAP), 1)

    def spread_row(x, j):
        return jnp.broadcast_to(x[j : j + 1, :], (8, SNAP))

    for b in range(16):
        full = m_ref[...]
        columns = [jnp.broadcast_to(full[:, 8 * b + j : 8 * b + j + 1], (SNAP, SNAP)) for j in range(8)]
        panel = full[8 * b : 8 * b + 8, :]
        pivots = [c[8 * b : 8 * b + 8, :] for c in columns]
        for j in range(8):
            own = sub == j
            inv = 1.0 / spread_row(pivots[j], j)
            pj = pivots[j]
            panel = jnp.where(lane == 8 * b + j, own.astype(jnp.float32), panel)
            new = spread_row(panel, j) * inv
            panel = jnp.where(own, new, panel - pj * new)
            for i in range(j + 1, 8):
                new = spread_row(pivots[i], j) * inv
                pivots[i] = jnp.where(own, new, pivots[i] - pj * new)
        inside = (lane >= 8 * b) & (lane < 8 * b + 8)
        spread = [spread_row(panel, j) for j in range(8)]
        for t in range(16):
            if t == b:
                m_ref[8 * t : 8 * t + 8, :] = panel
            else:
                rest = jnp.where(inside, 0.0, full[8 * t : 8 * t + 8, :])
                for j in range(8):
                    rest = rest - columns[j][8 * t : 8 * t + 8, :] * spread[j]
                m_ref[8 * t : 8 * t + 8, :] = rest
    return jnp.sqrt(energy)


def per_device(snapshots, base_flow):
    field = snapshots[0]
    f32, bf16 = jnp.float32, jnp.bfloat16
    vmem = pl.BlockSpec(memory_space=pltpu.VMEM)
    dma = pltpu.SemaphoreType.DMA
    slab_shape = field.shape
    cells = 64 * math.prod(slab_shape[1:])
    scale = 1.0 / math.sqrt(cells)
    modes = jax.ShapeDtypeStruct((32, 32, 128), bf16)
    dm, am = pl.pallas_call(
        functools.partial(kernel, scale),
        out_shape=(modes, modes),
        in_specs=[pl.BlockSpec(memory_space=pltpu.HBM)] * 2,
        out_specs=(vmem,) * 2,
        scratch_shapes=[
            pltpu.VMEM(slab_shape, bf16),
            pltpu.VMEM(base_flow.shape, f32),
            pltpu.VMEM(slab_shape, bf16),
            pltpu.VMEM(slab_shape, bf16),
            pltpu.VMEM((8,) + slab_shape[1:], bf16),
            pltpu.VMEM((4, 8, 128), f32),
            pltpu.VMEM((4, 8, 128), f32),
            pltpu.VMEM((10, 8, 128), f32),
            pltpu.VMEM((10, 8, 128), f32),
            pltpu.VMEM((512, 128), f32),
            pltpu.VMEM((CHUNKS, 4, 8, PER, 128), bf16),
            pltpu.VMEM((4, CHUNKS, 8, PER, 128), bf16),
            pltpu.VMEM((16, 3, 8, SNAP), f32),
            pltpu.VMEM((8, 3, 8, SNAP), f32),
            pltpu.VMEM((16, 3, 8, SNAP), f32),
            pltpu.VMEM((3, 8, SNAP), f32),
            pltpu.VMEM((8, 3, 8, SNAP), f32),
            pltpu.VMEM((3, 8, SNAP), f32),
            pltpu.VMEM((16, 3, 8, SNAP), f32),
            pltpu.VMEM((SNAP, SNAP), f32),
            pltpu.VMEM((3, SNAP, SNAP), bf16),
            pltpu.VMEM((2, 4, 8, 32, 128), bf16),
            dma((2,)),
            dma,
            dma,
            dma((2, CHUNKS)),
            dma((2, CHUNKS)),
            dma((2,)),
            dma((2,)),
            dma((16,)),
            dma((16,)),
            dma,
            dma,
            dma((CHUNKS, 4)),
            dma((4, CHUNKS)),
            dma((8,)),
            dma((16,)),
            dma((8,)),
            dma((8,)),
            dma((2, 16)),
            dma((16,)),
            dma((2, 4)),
            dma((2, 4)),
        ],
        compiler_params=pltpu.CompilerParams(
            collective_id=0, has_side_effects=True, vmem_limit_bytes=59 * MIB
        ),
        name="pod",
    )(field, base_flow)

    def placed(x):
        return x.reshape(4, 8, 32, 128).transpose(2, 0, 1, 3)

    return placed(dm), placed(am)


def solution(mesh):
    return jax.shard_map(
        per_device,
        mesh=mesh,
        in_specs=(P("grp", None, "slab", None, None), P("slab", None, None)),
        out_specs=(P("grp", "slab", None, None), P("grp", "slab", None, None)),
        check_vma=False,
    )
```

```python
import functools
import math

import jax
import jax.numpy as jnp
from jax import lax
from jax.experimental import pallas as pl
from jax.experimental.pallas import tpu as pltpu
from jax.sharding import PartitionSpec as P

SNAP = 128
SECTIONS = 4
CHUNKS = 8
PER = SNAP // CHUNKS
MESH = pl.DeviceIdType.MESH
MIB = 1 << 20

diffuse_x = 0.35
diffuse_side = 0.05
keep_center = 0.1
damping = 0.5


def remote(src, dst, send_sem, recv_sem, device):
    return pltpu.make_async_remote_copy(
        src_ref=src, dst_ref=dst, send_sem=send_sem, recv_sem=recv_sem, device_id=device, device_id_type=MESH
    )


def place():
    g = lax.axis_index("grp")
    s = lax.axis_index("slab")
    core = lax.rem(s, 2)
    plane = lax.rem(lax.div(s, 2), 16)
    zh = lax.div(s, 32)
    return g, s, core, plane, zh


def slab_of(zh, plane, core):
    return zh * 32 + plane * 2 + core


def kernel(
    scale,
    u_hbm,
    v_hbm,
    dm_ref,
    am_ref,
    u_ref,
    v_ref,
    left,
    right,
    relay_buf,
    vleft,
    vright,
    cp,
    cm,
    stage,
    own,
    quart,
    part,
    pair_buf,
    rs_buf,
    tile,
    zbuf,
    mine,
    coup_ref,
    m_ref,
    wide,
    terms,
    in_sem,
    c_send,
    c_recv,
    h_send,
    h_recv,
    v_send,
    v_recv,
    x_send,
    x_recv,
    y_send,
    y_recv,
    q_send,
    q_recv,
    p_send,
    p_recv,
    z_send,
    z_recv,
    g_send,
    g_recv,
    o_send,
    o_recv,
):
    g, s, core, plane, zh = place()
    ahead = lax.rem(s + 1, 64)
    back = lax.rem(s + 63, 64)
    adjoint = g == 3
    z = zh * 4 + g
    last = (plane == 15) & (core == 1)
    first = (plane == 0) & (core == 0)
    edge = last | first

    def at(depth, position, side):
        depth = lax.rem(depth, 8)
        return lax.rem(depth, 4), slab_of(lax.div(depth, 4), position, side)

    def plane_peer(d):
        return lax.rem(plane + d, 16)

    owner = lax.div(plane, 8) == core
    partner = (g, slab_of(zh, plane, 1 - core))
    loads = [
        pltpu.make_async_copy(v_hbm, v_ref, in_sem.at[0]),
        pltpu.make_async_copy(u_hbm, u_ref, in_sem.at[1]),
    ]
    for load in loads:
        load.start()
    barrier = pltpu.get_barrier_semaphore()

    def greet(device):
        pl.semaphore_signal(barrier, inc=1, device_id=device, device_id_type=MESH)

    greet((g, ahead))
    greet((g, back))
    greet(partner)
    for d in range(1, 16):
        for side in (core, 1 - core):
            greet((g, slab_of(zh, plane_peer(d), side)))
    for d in range(1, 8):
        greet(at(z + d, plane, core))
    far_end = at(z + 4, 15 * (1 - core), 1 - core)
    greet(far_end)

    @pl.when(edge)
    def _():
        def one(i, carry):
            greet(at(z + 4, i, 1 - core))
            return carry

        lax.fori_loop(0, 16, one, 0)

    for load in loads:
        load.wait()
    pl.semaphore_wait(barrier, 41 + jnp.where(edge, 16, 0))

    flow = [
        remote(v_ref, vleft, v_send.at[0], v_recv.at[0], (g, ahead)),
        remote(v_ref, vright, v_send.at[1], v_recv.at[1], (g, back)),
    ]
    for copy in flow:
        copy.start()

    def rows(c):
        return pl.ds(c * PER, PER)

    def halo(c):
        return [
            remote(u_ref.at[rows(c)], left.at[rows(c)], h_send.at[0, c], h_recv.at[0, c], (g, ahead)),
            remote(u_ref.at[rows(c)], right.at[rows(c)], h_send.at[1, c], h_recv.at[1, c], (g, back)),
        ]

    def half(i):
        return pl.ds(i * 8, 8)

    def to_relay(i):
        return remote(u_ref.at[half(i)], relay_buf, x_send.at[i], y_recv, (g, slab_of(zh, i, core)))

    def across(src, i, send_sem):
        return (
            remote(src, right.at[half(i)], send_sem, x_recv.at[i], far_end),
            remote(src, left.at[half(i)], send_sem, x_recv.at[i], far_end),
        )

    def start_across(src, i, send_sem):
        to_right, to_left = across(src, i, send_sem)

        @pl.when(core == 0)
        def _():
            to_right.start()

        @pl.when(core == 1)
        def _():
            to_left.start()

    @pl.when(edge)
    def _():
        def one(i, carry):
            @pl.when(i != plane)
            def _():
                to_relay(i).start()

            @pl.when(i == plane)
            def _():
                start_across(u_ref.at[half(i)], i, x_send.at[i])

            return carry

        lax.fori_loop(0, 16, one, 0)

    def start_halo(c, carry):
        ahead_copy, back_copy = halo(c)

        @pl.when(jnp.logical_not(last))
        def _():
            ahead_copy.start()

        @pl.when(jnp.logical_not(first))
        def _():
            back_copy.start()

        return carry

    lax.fori_loop(0, CHUNKS, start_halo, 0)

    def pass_on():
        pltpu.make_async_copy(relay_buf, relay_buf, y_recv).wait()
        start_across(relay_buf, plane, y_send)

    def halo_in(c):
        ahead_copy, back_copy = halo(c)

        @pl.when(jnp.logical_not(first))
        def _():
            ahead_copy.wait_recv()

        @pl.when(jnp.logical_not(last))
        def _():
            back_copy.wait_recv()

        @pl.when(edge)
        def _():
            for i in range(2):
                across(relay_buf, 2 * c + i, y_send)[0].wait_recv()

    for copy in flow:
        copy.wait()

    v = [vleft[k] for k in range(4)] + [v_ref[k] for k in range(4)] + [vright[k] for k in range(4)]
    for k in range(10):
        cp[k] = jnp.where(adjoint, diffuse_x + 0.5 * v[k + 2], diffuse_x - 0.5 * v[k + 1])
        cm[k] = jnp.where(adjoint, diffuse_x - 0.5 * v[k], diffuse_x + 0.5 * v[k + 1])

    def sections(snap, base):
        cells = [ref[snap, k].astype(jnp.float32) for ref in (left, u_ref, right) for k in range(4)]
        for section in range(SECTIONS):
            new = []
            for k in range(0, len(cells) - 2, 2):
                pair = jnp.concatenate([cells[k + 1], cells[k + 2]], axis=0).astype(jnp.bfloat16)
                lanes = (pltpu.roll(pair, 1, 1) + pltpu.roll(pair, 127, 1)).astype(jnp.float32)
                for j in range(2):
                    center = cells[k + 1 + j]
                    side = pltpu.roll(center, 1, 0) + pltpu.roll(center, 7, 0) + lanes[8 * j : 8 * j + 8]
                    new.append(
                        keep_center * center
                        + cp[section + k + j] * cells[k + j + 2]
                        + cm[section + k + j] * cells[k + j]
                        + diffuse_side * side
                    )
            cells = new
        for k in range(4):
            stage[pl.ds(base + k * 64, 8, stride=8), :] = cells[k]

    def piece(c, d):
        r = lax.rem(g + d, 4)
        return remote(own.at[c, r], quart.at[g, c], q_send.at[c, d], q_recv.at[g, c], (r, s))

    def piece_in(c, d):
        k = lax.rem(g + d, 4)
        return remote(own.at[c, k], quart.at[k, c], q_send.at[c, d], q_recv.at[k, c], (k, s))

    def chunk(c, carry):
        @pl.when(jnp.logical_not(edge) & (c == lax.div(plane + 2, 5)))
        def _():
            pass_on()

        halo_in(c)

        def one(part_no, inner):
            for i in range(8):
                sections(c * PER + part_no * 8 + i, part_no * 256 + i)
            return inner

        lax.fori_loop(0, 2, one, 0)

        def packed(q):
            low = stage[q * 8 : q * 8 + 8, :]
            high = stage[256 + q * 8 : 256 + q * 8 + 8, :]
            return jnp.concatenate([low, high], axis=0).astype(jnp.bfloat16)

        for q in range(32):
            own[c, q // 8, q % 8] = packed(q)
        odd = lax.rem(g, 2)
        for d in (2, 3 - 2 * odd, 1 + 2 * odd):
            piece(c, d).start()
        quart[g, c] = own[c, g]
        return carry

    lax.fori_loop(0, CHUNKS, chunk, 0)

    def gathered(c, carry):
        for d in range(1, 4):
            piece_in(c, d).wait_recv()
        return carry

    lax.fori_loop(0, CHUNKS, gathered, 0)

    def plane_device(p2, side):
        return g, slab_of(zh, p2, side)

    def swap():
        return remote(part.at[pl.ds((1 - core) * 8, 8)], pair_buf, c_send, c_recv, partner)

    def scatter(i):
        p2 = core * 8 + i
        return remote(part.at[p2], rs_buf.at[plane], p_send.at[i], p_recv.at[plane], plane_device(p2, core))

    def spread(d):
        return remote(tile, zbuf.at[z], z_send.at[d], z_recv.at[z], at(z + d, plane, core))

    def share(d, side):
        p2 = plane_peer(d)
        return remote(mine, coup_ref.at[plane], g_send.at[side, d], g_recv.at[plane], plane_device(p2, lax.rem(core + side, 2)))

    def landed(ref, sem, i, skip):
        @pl.when(jnp.logical_not(skip))
        def _():
            pltpu.make_async_copy(ref.at[i], ref.at[i], sem.at[i]).wait()

    def hops(d):
        return min(d // 4, 4 - d // 4) + min(d % 4, 4 - d % 4)

    others = [(d, side) for side in range(2) for d in range(16) if d or side]
    others.sort(key=lambda pair: -hops(pair[0]))

    def pair(k, q):
        return jnp.concatenate([quart[k, :, 2 * q + j].reshape(SNAP, 128) for j in range(2)], axis=1)

    def product(q, totals):
        lhs = pair(3, q)
        wide_two = jnp.concatenate([pair(0, q), pair(1, q)], axis=0)

        def against(rhs):
            return lax.dot_general(lhs, rhs, (((1,), (1,)), ((), ())), preferred_element_type=jnp.float32)

        return totals[0] + against(wide_two), totals[1] + against(pair(2, q))

    two, one_more = lax.fori_loop(
        0, 4, product, (jnp.zeros((SNAP, 2 * SNAP), jnp.float32), jnp.zeros((SNAP, SNAP), jnp.float32))
    )
    for k, total in enumerate((two[:, :SNAP], two[:, SNAP:], one_more)):
        part[:, k] = total.reshape(16, 8, SNAP)
    swap().start()
    swap().wait_recv()
    for i in range(8):
        p2 = core * 8 + i
        part[p2] += pair_buf[i]

        @pl.when(p2 != plane)
        def _():
            scatter(i).start()

    @pl.when(owner)
    def _():
        rs_buf[plane] = part[plane]
        for i in range(16):
            landed(rs_buf, p_recv, i, plane == i)
        tile[...] = jnp.sum(rs_buf[...], axis=0)
        for d in range(1, 8):
            spread(d).start()
        zbuf[z] = tile[...]
        for i in range(8):
            landed(zbuf, z_recv, i, z == i)
        mine[...] = jnp.sum(zbuf[...], axis=0) * scale
        for d, side in others:
            share(d, side).start()
        coup_ref[plane] = mine[...]

    for i in range(16):
        landed(coup_ref, g_recv, i, owner & (plane == i))

    root = invert(coup_ref, m_ref)

    def post(d, kind):
        r = lax.rem(g + d, 4)
        out = (dm_ref, am_ref)[kind]
        here = pl.ds(pl.multiple_of(g * 8, 8), 8)
        return remote(terms.at[kind, r], out.at[here], o_send.at[kind, d], o_recv.at[kind, g], (r, s))

    def post_in(d, kind):
        k = lax.rem(g + d, 4)
        out = (dm_ref, am_ref)[kind]
        there = pl.ds(pl.multiple_of(k * 8, 8), 8)
        return remote(terms.at[kind, k], out.at[there], o_send.at[kind, d], o_recv.at[kind, k], (k, s))

    def modes(kind, value):
        def one(q, carry):
            x = value(q).astype(jnp.bfloat16)
            for j in range(2):
                terms[kind, :, 2 * q + j] = x[:, j * 128 : j * 128 + 128].reshape(4, 32, 128)
            return carry

        lax.fori_loop(0, 4, one, 0)
        for d in (2, 3, 1):
            post(d, kind).start()
        here = pl.ds(pl.multiple_of(g * 8, 8), 8)
        (dm_ref, am_ref)[kind][here] = terms[kind, g]

    inverse = m_ref[...].astype(jnp.bfloat16)
    modes(1, lambda q: jnp.dot(inverse, pair(3, q), preferred_element_type=jnp.float32))
    for k in range(3):
        wide[k] = (
            jnp.dot(
                m_ref[...],
                coup_ref[:, k].reshape(SNAP, SNAP),
                precision=lax.Precision.HIGHEST,
                preferred_element_type=jnp.float32,
            )
            / root
        ).astype(jnp.bfloat16)

    def direct_value(q):
        total = jnp.dot(wide[0], pair(0, q), preferred_element_type=jnp.float32)
        for k in (1, 2):
            total = total + jnp.dot(wide[k], pair(k, q), preferred_element_type=jnp.float32)
        return total

    modes(0, direct_value)
    for kind in (1, 0):
        for d in range(1, 4):
            post_in(d, kind).wait_recv()

    def drain(c, carry):
        ahead_copy, back_copy = halo(c)

        @pl.when(jnp.logical_not(last))
        def _():
            ahead_copy.wait_send()

        @pl.when(jnp.logical_not(first))
        def _():
            back_copy.wait_send()

        for d in range(1, 4):
            piece(c, d).wait_send()
        return carry

    lax.fori_loop(0, CHUNKS, drain, 0)

    @pl.when(edge)
    def _():
        def one(i, carry):
            to_relay(i).wait_send()
            return carry

        lax.fori_loop(0, 16, one, 0)

    @pl.when(jnp.logical_not(edge))
    def _():
        across(relay_buf, plane, y_send)[0].wait_send()

    swap().wait_send()
    for i in range(8):

        @pl.when(core * 8 + i != plane)
        def _():
            scatter(i).wait_send()

    @pl.when(owner)
    def _():
        for d in range(1, 8):
            spread(d).wait_send()
        for d, side in others:
            share(d, side).wait_send()

    for kind in range(2):
        for d in range(1, 4):
            post(d, kind).wait_send()


def invert(coup_ref, m_ref):
    gram = jnp.zeros((SNAP, SNAP), jnp.float32)
    for k in range(3):
        c = coup_ref[:, k].reshape(SNAP, SNAP)
        gram = gram + lax.dot_general(
            c, c, (((1,), (1,)), ((), ())), precision=lax.Precision.HIGHEST, preferred_element_type=jnp.float32
        )
    row = lax.broadcasted_iota(jnp.int32, (SNAP, SNAP), 0)
    col = lax.broadcasted_iota(jnp.int32, (SNAP, SNAP), 1)
    eye = (row == col).astype(jnp.float32)
    energy = jnp.sum(gram * eye, axis=(0, 1), keepdims=True) / SNAP
    m_ref[...] = gram / energy + damping * eye

    sub = lax.broadcasted_iota(jnp.int32, (8, SNAP), 0)
    lane = lax.broadcasted_iota(jnp.int32, (8, SNAP), 1)

    def spread_row(x, j):
        return jnp.broadcast_to(x[j : j + 1, :], (8, SNAP))

    for b in range(16):
        full = m_ref[...]
        columns = [jnp.broadcast_to(full[:, 8 * b + j : 8 * b + j + 1], (SNAP, SNAP)) for j in range(8)]
        panel = full[8 * b : 8 * b + 8, :]
        pivots = [c[8 * b : 8 * b + 8, :] for c in columns]
        for j in range(8):
            own = sub == j
            inv = 1.0 / spread_row(pivots[j], j)
            pj = pivots[j]
            panel = jnp.where(lane == 8 * b + j, own.astype(jnp.float32), panel)
            new = spread_row(panel, j) * inv
            panel = jnp.where(own, new, panel - pj * new)
            for i in range(j + 1, 8):
                new = spread_row(pivots[i], j) * inv
                pivots[i] = jnp.where(own, new, pivots[i] - pj * new)
        inside = (lane >= 8 * b) & (lane < 8 * b + 8)
        spread = [spread_row(panel, j) for j in range(8)]
        for t in range(16):
            if t == b:
                m_ref[8 * t : 8 * t + 8, :] = panel
            else:
                rest = jnp.where(inside, 0.0, full[8 * t : 8 * t + 8, :])
                for j in range(8):
                    rest = rest - columns[j][8 * t : 8 * t + 8, :] * spread[j]
                m_ref[8 * t : 8 * t + 8, :] = rest
    return jnp.sqrt(energy)


def per_device(snapshots, base_flow):
    field = snapshots[0]
    f32, bf16 = jnp.float32, jnp.bfloat16
    vmem = pl.BlockSpec(memory_space=pltpu.VMEM)
    dma = pltpu.SemaphoreType.DMA
    slab_shape = field.shape
    cells = 64 * math.prod(slab_shape[1:])
    scale = 1.0 / math.sqrt(cells)
    modes = jax.ShapeDtypeStruct((32, 32, 128), bf16)
    dm, am = pl.pallas_call(
        functools.partial(kernel, scale),
        out_shape=(modes, modes),
        in_specs=[pl.BlockSpec(memory_space=pltpu.HBM)] * 2,
        out_specs=(vmem,) * 2,
        scratch_shapes=[
            pltpu.VMEM(slab_shape, bf16),
            pltpu.VMEM(base_flow.shape, f32),
            pltpu.VMEM(slab_shape, bf16),
            pltpu.VMEM(slab_shape, bf16),
            pltpu.VMEM((8,) + slab_shape[1:], bf16),
            pltpu.VMEM((4, 8, 128), f32),
            pltpu.VMEM((4, 8, 128), f32),
            pltpu.VMEM((10, 8, 128), f32),
            pltpu.VMEM((10, 8, 128), f32),
            pltpu.VMEM((512, 128), f32),
            pltpu.VMEM((CHUNKS, 4, 8, PER, 128), bf16),
            pltpu.VMEM((4, CHUNKS, 8, PER, 128), bf16),
            pltpu.VMEM((16, 3, 8, SNAP), f32),
            pltpu.VMEM((8, 3, 8, SNAP), f32),
            pltpu.VMEM((16, 3, 8, SNAP), f32),
            pltpu.VMEM((3, 8, SNAP), f32),
            pltpu.VMEM((8, 3, 8, SNAP), f32),
            pltpu.VMEM((3, 8, SNAP), f32),
            pltpu.VMEM((16, 3, 8, SNAP), f32),
            pltpu.VMEM((SNAP, SNAP), f32),
            pltpu.VMEM((3, SNAP, SNAP), bf16),
            pltpu.VMEM((2, 4, 8, 32, 128), bf16),
            dma((2,)),
            dma,
            dma,
            dma((2, CHUNKS)),
            dma((2, CHUNKS)),
            dma((2,)),
            dma((2,)),
            dma((16,)),
            dma((16,)),
            dma,
            dma,
            dma((CHUNKS, 4)),
            dma((4, CHUNKS)),
            dma((8,)),
            dma((16,)),
            dma((8,)),
            dma((8,)),
            dma((2, 16)),
            dma((16,)),
            dma((2, 4)),
            dma((2, 4)),
        ],
        compiler_params=pltpu.CompilerParams(
            collective_id=0, has_side_effects=True, vmem_limit_bytes=59 * MIB
        ),
        name="pod",
    )(field, base_flow)

    def placed(x):
        return x.reshape(4, 8, 32, 128).transpose(2, 0, 1, 3)

    return placed(dm), placed(am)


def solution(mesh):
    return jax.shard_map(
        per_device,
        mesh=mesh,
        in_specs=(P("grp", None, "slab", None, None), P("slab", None, None)),
        out_specs=(P("grp", "slab", None, None), P("grp", "slab", None, None)),
        check_vma=False,
    )
```
